32 devices in a mesh: tm: 8 (over z, y), space: 4 (over x, core).
Axes of the slice: x: 2, y: 2, z: 4, core: 2. Of those that a mesh axis runs over, the one named last changes fastest.
Arguments:
- increments: float32 [8, 3, 512, 1024], P('tm', None, 'space'), may hold values from -6 to 6
- start_state: float32 [3, 512, 1024], P(None, 'space'), may hold values from -6 to 6
- depth: float32 [512, 1024], P('space'), may hold values from 0.5 to 1.5
- error_weight: float32 [3, 512, 1024], P(None, 'space'), may hold values from 0.25 to 1
- obs_index: int32 [8, 4096], P('tm'), may hold values from 0 to 1572863
- obs_count: int32 [8], P('tm'), may hold values from 1024 to 4096, as said below
- obs_value: float32 [8, 4096], P('tm'), may hold values from -6 to 6
- obs_weight: float32 [8, 4096], P('tm'), may hold values from 0.5 to 2
Outputs:
- analysis: float32 [8, 3, 512, 1024], P('tm', None, 'space')
- costs: float32 [2, 8], P(None, 'tm')
The draws below stay inside these ranges and needn't reach their ends.
Inputs may be any that keep to these rules, and one draw needn't show every extreme that they name: Only the first obs_count entries of a subwindow's observation rows are live; some subwindow has all 4096 live.
All inputs are finite; a program needn't handle non-finite values.
Results may differ from the reference program's by a relative error of at most 0.0001.
Values sent between devices are 32-bit elements; how exact they have to be, the bound alone decides.
No kernel may reach another device: no remote copies, remote signals or barrier semaphores. Data moves between devices by JAX's collectives and lax.ppermute only.
A program may use at most 128 MiB of HBM per device.

```python
import math
import jax
import jax.numpy as jnp

LON = 1024
NOBS = 4096
STEPS = 6
ITERS = 2
SUBWIN = 8
LAT = 512


def draw_obs_count(key, part):
    first_key, second_key = jax.random.split(jax.random.fold_in(key, 17))
    counted = jax.random.randint(first_key, (SUBWIN,), NOBS // 4, NOBS + 1)
    position = jax.random.randint(second_key, (), 0, SUBWIN)
    return counted.at[position].set(NOBS).astype(jnp.int32)


def touch_ends(entries, own_key, least, top_value):
    longest = entries.shape.index(max(entries.shape))
    spots = []
    for shift in (0, 1):
        where = [jax.random.randint(jax.random.fold_in(own_key, axis), (), 0, length) for axis, length in enumerate(entries.shape)]
        where[longest] = (where[longest] + shift) % entries.shape[longest]
        spots.append(tuple(where))
    return entries.at[spots[0]].set(least).at[spots[1]].set(top_value)


def shard_levels(key, shape, cuts, smallest, largest):
    factor_of, own = 1.0, jax.random.fold_in(key, 6)
    for dim, parts in cuts:
        steps = jnp.exp(jax.random.uniform(jax.random.fold_in(own, dim), (parts,), jnp.float32, smallest / len(cuts), largest / len(cuts)))
        factor_of = factor_of * jnp.repeat(steps, shape[dim] // parts).reshape([-1 if axis == dim else 1 for axis in range(len(shape))])
    return factor_of


def noise(stream_key, dims, width, bound, pieces=(), held_as=jnp.bfloat16):
    drawn = jax.random.normal(stream_key, dims, jnp.float32) * width
    if len(pieces) > 0:
        drawn = shard_levels(stream_key, dims, pieces, -0.22, 0.18) * drawn
    return jnp.clip(drawn, min=-bound, max=bound).astype(held_as)


def setup_inputs(seed: int = 0) -> dict:
    streams_of = jax.random.split(jax.random.key(seed), 9)
    return {
        "increments": noise(streams_of[0], (SUBWIN, 3, LAT, LON), 1.0, 6.0, ((0, 8), (2, 4)), jnp.float32),
        "start_state": noise(streams_of[1], (3, LAT, LON), 1.0, 6.0, ((1, 4),), jnp.float32),
        "depth": jnp.clip(jnp.exp(math.log(1.5) - 1.0986123 * jax.random.uniform(streams_of[2], (LAT, LON), jnp.float32) ** shard_levels(streams_of[2], (LAT, LON), ((0, 4),), -0.2, 0.2)), 0.5, 1.5),
        "error_weight": jnp.clip(jnp.exp(math.log(1.0) - 1.3862944 * jax.random.uniform(streams_of[3], (3, LAT, LON), jnp.float32) ** shard_levels(streams_of[3], (3, LAT, LON), ((1, 4),), -0.2, 0.2)), 0.25, 1.0),
        "obs_index": touch_ends(jax.random.randint(streams_of[4], (SUBWIN, NOBS), 0, 3 * LAT * LON), jax.random.fold_in(streams_of[4], 1), 0, (3 * LAT * LON) - 1).astype(jnp.int32),
        "obs_count": draw_obs_count(jax.random.fold_in(streams_of[8], 71), 0),
        "obs_value": noise(streams_of[6], (SUBWIN, NOBS), 1.0, 6.0, ((0, 8),), jnp.float32),
        "obs_weight": jnp.clip(jnp.exp(math.log(2.0) - 1.3862944 * jax.random.uniform(streams_of[7], (SUBWIN, NOBS), jnp.float32) ** shard_levels(streams_of[7], (SUBWIN, NOBS), ((0, 8),), -0.2, 0.2)), 0.5, 2.0),
    }


COURANT = 0.35
CORIOLIS_MAX = 0.2
STEP_SIZE = 0.2


def coriolis(total_rows, first_row, row_count):
    latitude = ((first_row + jnp.arange(row_count)).astype(jnp.float32) + 0.5) / total_rows * math.pi - math.pi / 2
    return (CORIOLIS_MAX * jnp.sin(latitude))[:, None]


def diff_lon(field):
    return (jnp.roll(field, -1, -1) - jnp.roll(field, 1, -1)) * 0.5


def diff_lat(field):
    widths = [(0, 0)] * (field.ndim - 2) + [(1, 1), (0, 0)]
    padded = jnp.pad(field, widths)
    return (padded[..., 2:, :] - padded[..., :-2, :]) * 0.5


def forward_model(state, depth, rate):
    zonal, merid, height = state[:, 0], state[:, 1], state[:, 2]
    for step in range(STEPS):
        height = height - COURANT * (diff_lon(depth * zonal) + diff_lat(depth * merid))
        zonal = zonal + rate * merid - COURANT * diff_lon(height)
        merid = merid - rate * zonal - COURANT * diff_lat(height)
    return jnp.stack([zonal, merid, height], 1)


def adjoint_model(state, depth, rate):
    adj_zonal, adj_merid, adj_height = state[:, 0], state[:, 1], state[:, 2]
    for step in range(STEPS):
        zonal_mix = adj_zonal - rate * adj_merid
        height_mix = adj_height + COURANT * diff_lat(adj_merid) + COURANT * diff_lon(zonal_mix)
        adj_zonal = zonal_mix + COURANT * depth * diff_lon(height_mix)
        adj_merid = adj_merid + rate * zonal_mix + COURANT * depth * diff_lat(height_mix)
        adj_height = height_mix
    return jnp.stack([adj_zonal, adj_merid, adj_height], 1)


def reference(increments, start_state, depth, error_weight, obs_index, obs_count, obs_value, obs_weight):
    rate = coriolis(LAT, 0, LAT)
    state = increments
    cells = 3 * LAT * LON
    is_live = jnp.arange(NOBS)[None, :] < obs_count[:, None]

    def deposit(where_idx, values):
        return jnp.zeros((cells,), jnp.float32).at[where_idx].add(values)

    cost_list = []
    for sweep_index in range(ITERS):
        endpoints = forward_model(state, depth, rate)
        previous = jnp.concatenate([start_state[None], endpoints[:-1]], 0)
        model_gap = state - previous
        weighted_gap = error_weight * model_gap
        back_image = jnp.concatenate([adjoint_model(weighted_gap[1:], depth, rate), jnp.zeros_like(weighted_gap[:1])], 0)
        flattened = state.reshape(state.shape[0], -1)
        observed = jnp.take_along_axis(flattened, obs_index, 1)
        resid = jnp.where(is_live, observed - obs_value, 0.0)
        weighted = obs_weight * resid
        obs_grad = jax.vmap(deposit)(obs_index, weighted).reshape(state.shape)
        cost_now = (0.5 * jnp.sum(weighted_gap * model_gap, (1, 2, 3)) + 0.5 * jnp.sum(weighted * resid, 1)) / cells
        cost_list.append(cost_now)
        state = state - STEP_SIZE * (weighted_gap - back_image + obs_grad)
    return state, jnp.stack(cost_list, 0)
```

```python
import math

import jax
import jax.numpy as jnp
from jax import lax
from jax.experimental import pallas as pl
from jax.experimental.pallas import tpu as pltpu
from jax.sharding import PartitionSpec as P

STEPS = 6
ITERS = 2
COURANT = 0.35
CORIOLIS_MAX = 0.2
STEP_SIZE = 0.2

SUB = 8
LANE = 128
NEAR = 16
FAR = 24
GROUPS = 4
HALF = 0.5 * COURANT


def tile_rows(i):
    return pl.ds(SUB * i, SUB)


def wide(tile, width):
    return jnp.concatenate([tile] * (width // LANE), axis=1)


def raw_lon(x):
    width = x.shape[1]
    return pltpu.roll(x, width - 1, 1) - pltpu.roll(x, 1, 1)


class LatDiff:
    def __init__(self, count, width):
        row = lax.broadcasted_iota(jnp.int32, (SUB, width), 0)
        self.first, self.last = row == 0, row == SUB - 1
        self.count, self.up, self.down = count, {}, {}

    def put(self, i, x):
        self.up[i] = pltpu.roll(x, SUB - 1, 0)
        self.down[i] = pltpu.roll(x, 1, 0)

    def at(self, i):
        above = self.up[min(i + 1, self.count - 1)]
        below = self.down[max(i - 1, 0)]
        return jnp.where(self.last, above, self.up[i]) - jnp.where(
            self.first, below, self.down[i]
        )


def sweep(state, depth, rate, off, halo, edge_ref, forward):
    count = state.shape[1] // SUB
    width = state.shape[2]
    north, south = halo // SUB - 1, count - halo // SUB

    def one(_, carry):
        first, second = LatDiff(count, width), LatDiff(count, width)

        def coef(i):
            return depth[pl.ds(off + SUB * i, SUB), :]

        def rot(i):
            return wide(rate[pl.ds(off + SUB * i, SUB), :], width)

        def masked(i, x):
            if i == north:
                return x * edge_ref[0]
            if i == south:
                return x * edge_ref[1]
            return x

        def prepare(i):
            v = state[1, tile_rows(i), :]
            first.put(i, coef(i) * v if forward else v)

        def stage_a(i):
            if i + 1 < count:
                prepare(i + 1)
            if forward:
                flow = coef(i) * state[0, tile_rows(i), :]
                new = state[2, tile_rows(i), :] - (raw_lon(flow) + first.at(i))
            else:
                mix = state[0, tile_rows(i), :] - rot(i) * state[1, tile_rows(i), :]
                state[0, tile_rows(i), :] = mix
                new = state[2, tile_rows(i), :] + (raw_lon(mix) + first.at(i))
            new = masked(i, new)
            state[2, tile_rows(i), :] = new
            second.put(i, new)

        def stage_b(i):
            new = state[2, tile_rows(i), :]
            u, v = state[0, tile_rows(i), :], state[1, tile_rows(i), :]
            if forward:
                u = u + rot(i) * v - raw_lon(new)
                v = v - rot(i) * u - second.at(i)
                state[0, tile_rows(i), :] = u
                state[1, tile_rows(i), :] = v
            else:
                state[0, tile_rows(i), :] = u + coef(i) * raw_lon(new)
                state[1, tile_rows(i), :] = v + rot(i) * u + coef(i) * second.at(i)

        prepare(0)
        for i in range(count):
            stage_a(i)
            if i > 0:
                stage_b(i - 1)
        stage_b(count - 1)
        return carry

    lax.fori_loop(0, STEPS, one, 0)


def gap_kernel(
    own_lo,
    flags,
    own_e,
    own_m,
    mid_e,
    mid_m,
    far_e,
    far_m,
    from_north,
    from_south,
    start,
    depth,
    rate,
    weight,
    obs_a,
    obs_b,
    lam_out,
    part_out,
    cost_out,
    lo,
    mid,
    kept,
    hi,
    depth_v,
    rate_v,
    weight_v,
    a_v,
    b_v,
    sems,
):
    rows = kept.shape[1]
    inner = rows - 2 * FAR
    width = kept.shape[2]

    def assemble(dst, halo, e, m, at, slot):
        pieces = [
            (from_north.at[:, pl.ds(at, halo), :], 0, halo),
            (e.at[:, pl.ds(0, FAR), :], halo, FAR),
            (m, halo + FAR, inner),
            (e.at[:, pl.ds(FAR, FAR), :], halo + FAR + inner, FAR),
            (from_south.at[:, pl.ds(at, halo), :], halo + rows, halo),
        ]
        return [
            pltpu.make_async_copy(src, dst.at[:, pl.ds(where, size), :], sems.at[slot + n])
            for n, (src, where, size) in enumerate(pieces)
        ]

    own_at, mid_at, far_at = 0, NEAR, NEAR + FAR
    is_own_lo = own_lo[0] == 1
    c_depth = pltpu.make_async_copy(depth, depth_v, sems.at[0])
    c_rate = pltpu.make_async_copy(rate, rate_v, sems.at[1])
    c_mid = assemble(mid, FAR, mid_e, mid_m, mid_at, 2)
    lo_own = assemble(lo, NEAR, own_e, own_m, own_at, 7)
    lo_far = assemble(lo, NEAR, far_e, far_m, far_at, 7)
    hi_own = assemble(hi, NEAR, own_e, own_m, own_at, 12)
    hi_far = assemble(hi, NEAR, far_e, far_m, far_at, 12)
    c_kept = [
        pltpu.make_async_copy(mid_e.at[:, pl.ds(0, FAR), :], kept.at[:, pl.ds(0, FAR), :], sems.at[17]),
        pltpu.make_async_copy(mid_m, kept.at[:, pl.ds(FAR, inner), :], sems.at[18]),
        pltpu.make_async_copy(
            mid_e.at[:, pl.ds(FAR, FAR), :], kept.at[:, pl.ds(FAR + inner, FAR), :], sems.at[19]
        ),
    ]
    c_weight = pltpu.make_async_copy(weight, weight_v, sems.at[20])
    c_a = pltpu.make_async_copy(obs_a, a_v, sems.at[21])
    c_b = pltpu.make_async_copy(obs_b, b_v, sems.at[22])
    c_depth.start()
    c_rate.start()
    for c in c_mid:
        c.start()

    @pl.when(is_own_lo)
    def _():
        for c in lo_own + hi_far:
            c.start()

    @pl.when(jnp.logical_not(is_own_lo))
    def _():
        for c in lo_far + hi_own:
            c.start()

    for c in c_kept + [c_weight, c_a, c_b]:
        c.start()

    c_depth.wait()
    c_rate.wait()
    for c in c_mid:
        c.wait()

    def scale_third(ref, factor):
        for i in range(ref.shape[1] // SUB):
            ref[2, tile_rows(i), :] = ref[2, tile_rows(i), :] * factor

    scale_third(mid, HALF)
    sweep(mid, depth_v, rate_v, 0, FAR, flags, True)
    for c in lo_own:
        c.wait()

    scale_third(lo, HALF)
    sweep(lo, depth_v, rate_v, FAR - NEAR, NEAR, flags, True)
    for c in hi_own + [c_weight]:
        c.wait()

    for part in range(3):
        back_scale = 1.0 / HALF if part == 2 else 1.0
        for i in range(lam_out.shape[1] // SUB):
            end = mid[part, pl.ds(FAR - NEAR + SUB * i, SUB), :] * back_scale
            lam = weight_v[part, tile_rows(i), :] * (hi[part, tile_rows(i), :] - end)
            lam_out[part, tile_rows(i), :] = lam * (flags[2] * back_scale)

    for c in c_kept + [c_a, c_b]:
        c.wait()

    @pl.when(flags[3] > 0.5)
    def _():
        c = pltpu.make_async_copy(start, lo.at[:, pl.ds(NEAR, rows), :], sems.at[0])
        c.start()
        c.wait()
        for i in range(rows // SUB):
            at = pl.ds(NEAR + SUB * i, SUB)
            lo[2, at, :] = lo[2, at, :] * HALF

    model = jnp.zeros((SUB, width), jnp.float32)
    fit = jnp.zeros((SUB, width), jnp.float32)
    for part in range(3):
        back_scale = 1.0 / HALF if part == 2 else 1.0
        for i in range(rows // SUB):
            here = kept[part, tile_rows(i), :]
            near = pl.ds(NEAR + SUB * i, SUB)
            gap = here - lo[part, near, :] * back_scale
            lam = weight_v[part, near, :] * gap
            pull = a_v[part, tile_rows(i), :] * here
            model = model + lam * gap
            fit = fit + here * (pull - 2.0 * b_v[part, tile_rows(i), :])
            part_out[part, tile_rows(i), :] = here - STEP_SIZE * (
                lam + (pull - b_v[part, tile_rows(i), :])
            )
    total = model + fit
    folded = total[:, :LANE]
    for n in range(1, width // LANE):
        folded = folded + total[:, n * LANE : (n + 1) * LANE]
    cost_out[...] = folded


def step_kernel(flags, lam, part, depth, rate, edge_out, mid_out, work):
    rows, width = part.shape[1], part.shape[2]
    work[...] = lam[...]
    sweep(work, depth, rate, FAR - NEAR, NEAR, flags, False)
    for c in range(3):
        scale = STEP_SIZE * (HALF if c == 2 else 1.0)
        for i in range(rows // SUB):
            new = part[c, tile_rows(i), :] + scale * work[c, pl.ds(NEAR + SUB * i, SUB), :]
            if SUB * i < FAR:
                edge_out[c, tile_rows(i), :] = new
            elif SUB * i < rows - FAR:
                mid_out[c, pl.ds(SUB * i - FAR, SUB), :] = new
            else:
                edge_out[c, pl.ds(SUB * i - rows + 2 * FAR, SUB), :] = new


def final_kernel(flags, lam, part, depth, rate, out, work):
    rows = part.shape[1]
    work[...] = lam[...]
    sweep(work, depth, rate, FAR - NEAR, NEAR, flags, False)
    for c in range(3):
        scale = STEP_SIZE * (HALF if c == 2 else 1.0)
        for i in range(rows // SUB):
            out[c, tile_rows(i), :] = (
                part[c, tile_rows(i), :] + scale * work[c, pl.ds(NEAR + SUB * i, SUB), :]
            )


def deposit_kernel(code, load, value, a_out, b_out, *acc):
    a_acc, b_acc = acc[:GROUPS], acc[GROUPS:]
    chunks = a_out.shape[1] // LANE
    zero = jnp.zeros((SUB, LANE), jnp.float32)
    rows = a_out.shape[0]

    def clear(r, c):
        for ref in acc:
            for n in range(SUB):
                ref[pl.ds(pl.multiple_of((r * SUB + n) * SUB, SUB), SUB), :] = zero
        return c

    lax.fori_loop(0, rows // SUB, clear, 0)
    column = lax.broadcasted_iota(jnp.int32, (SUB, LANE), 0) * LANE + lax.broadcasted_iota(
        jnp.int32, (SUB, LANE), 1
    )
    shift = (chunks * LANE).bit_length() - 1

    def body(n, c):
        for g in range(GROUPS):
            i = n * GROUPS + g
            word = code[i]
            at = pl.ds(pl.multiple_of((word >> shift) * SUB, SUB), SUB)
            hit = column == (word & (chunks * LANE - 1))
            a_acc[g][at, :] = a_acc[g][at, :] + jnp.where(hit, load[i], 0.0)
            b_acc[g][at, :] = b_acc[g][at, :] + jnp.where(hit, value[i], 0.0)
        return c

    lax.fori_loop(0, code.shape[0] // GROUPS, body, 0, unroll=4)

    def gather(t, c):
        at = pl.ds(pl.multiple_of(t * SUB, SUB), SUB)
        for s in range(chunks):
            def total(refs):
                picked = [ref[pl.ds(t * SUB * SUB + s, SUB, stride=SUB), :] for ref in refs]
                return (picked[0] + picked[1]) + (picked[2] + picked[3])

            a_out[at, pl.ds(s * LANE, LANE)] = total(a_acc)
            b_out[at, pl.ds(s * LANE, LANE)] = total(b_acc)
        return c

    lax.fori_loop(0, rows // SUB, gather, 0)


def per_device(
    increments, start_state, depth, error_weight, obs_index, obs_count, obs_value, obs_weight
):
    _, comps, rows, lon = increments.shape
    bands = lax.axis_size("space")
    windows = lax.axis_size("tm")
    band = lax.axis_index("space")
    me = lax.axis_index("tm")
    even = me % 2 == 0
    total_rows = rows * bands
    first_row = band * rows
    f32 = jnp.float32
    any_space = pl.BlockSpec(memory_space=pl.ANY)
    smem = pl.BlockSpec(memory_space=pltpu.SMEM)
    vmem = pl.BlockSpec(memory_space=pltpu.VMEM)

    swap = [(i, i ^ 1) for i in range(windows)]
    inward = [(i, i - 2) for i in range(2, windows) if i % 2 == 0] + [
        (i, i + 2) for i in range(windows - 2) if i % 2 == 1
    ]
    outward = [(b, a) for a, b in inward]
    southward = [(i, i + 1) for i in range(bands - 1)]
    northward = [(b, a) for a, b in southward]

    index = obs_index[0]
    plane = total_rows * lon
    component = index // plane
    remainder = index % plane
    local = remainder // lon - first_row
    kept = (local >= 0) & (local < rows) & (jnp.arange(index.shape[0]) < obs_count[0])
    code = jnp.where(kept, (component * rows + local) * lon + remainder % lon, comps * rows * lon)
    load = jnp.where(kept, obs_weight[0], 0.0)
    pulled = load * obs_value[0]
    own_list = jnp.stack([code.astype(f32), load, pulled])
    own_const = jnp.sum(pulled * obs_value[0])
    other_list = lax.ppermute(own_list, "tm", swap)

    deposit = pl.pallas_call(
        deposit_kernel,
        in_specs=[smem] * 3,
        out_specs=[vmem] * 2,
        out_shape=[jax.ShapeDtypeStruct((comps * rows, lon), f32)] * 2,
        scratch_shapes=[pltpu.VMEM(((comps * rows + SUB) * SUB, LANE), f32)] * (2 * GROUPS),
        cost_estimate=pl.CostEstimate(flops=40_000_000, bytes_accessed=0, transcendentals=0),
        name="deposit",
    )

    def deposited(words, scale, value):
        a, b = deposit(words, scale, value)
        return a.reshape(comps, rows, lon), b.reshape(comps, rows, lon)

    def beside(block, size):
        return block[:, rows - size :], block[:, :size]

    weight_s, weight_n = beside(error_weight, NEAR)
    depth_s, depth_n = beside(depth[None], FAR)
    flat = lambda w, d: jnp.concatenate([w.reshape(-1, lon), d[0]], 0)
    const_n = lax.ppermute(flat(weight_s, depth_s), "space", southward)
    const_s = lax.ppermute(flat(weight_n, depth_n), "space", northward)
    split = comps * NEAR
    shaped = lambda c: c[:split].reshape(comps, NEAR, lon)
    weight_wide = jnp.concatenate([shaped(const_n), error_weight, shaped(const_s)], 1)
    depth_wide = (HALF * HALF) * jnp.concatenate([const_n[split:], depth, const_s[split:]], 0)
    latitude = (
        (first_row - FAR + jnp.arange(rows + 2 * FAR)).astype(f32) + 0.5
    ) / total_rows * math.pi - math.pi / 2
    rate_wide = jnp.broadcast_to(
        (CORIOLIS_MAX * jnp.sin(latitude))[:, None], (rows + 2 * FAR, LANE)
    )

    near_rows, far_rows = rows + 2 * NEAR, rows + 2 * FAR
    gap_call = pl.pallas_call(
        gap_kernel,
        in_specs=[smem, smem] + [any_space] * 14,
        out_specs=[vmem] * 3,
        out_shape=[
            jax.ShapeDtypeStruct((comps, near_rows, lon), f32),
            jax.ShapeDtypeStruct((comps, rows, lon), f32),
            jax.ShapeDtypeStruct((SUB, LANE), f32),
        ],
        scratch_shapes=[
            pltpu.VMEM((comps, near_rows, lon), f32),
            pltpu.VMEM((comps, far_rows, lon), f32),
            pltpu.VMEM((comps, rows, lon), f32),
            pltpu.VMEM((comps, near_rows, lon), f32),
            pltpu.VMEM((far_rows, lon), f32),
            pltpu.VMEM((far_rows, LANE), f32),
            pltpu.VMEM((comps, near_rows, lon), f32),
            pltpu.VMEM((comps, rows, lon), f32),
            pltpu.VMEM((comps, rows, lon), f32),
            pltpu.SemaphoreType.DMA((23,)),
        ],
        cost_estimate=pl.CostEstimate(flops=30_000_000, bytes_accessed=0, transcendentals=0),
        name="gaps",
    )
    step_cost = pl.CostEstimate(flops=15_000_000, bytes_accessed=0, transcendentals=0)
    step_call = pl.pallas_call(
        step_kernel,
        in_specs=[smem] + [vmem] * 4,
        out_specs=[vmem] * 2,
        out_shape=[
            jax.ShapeDtypeStruct((comps, 2 * FAR, lon), f32),
            jax.ShapeDtypeStruct((comps, rows - 2 * FAR, lon), f32),
        ],
        scratch_shapes=[pltpu.VMEM((comps, near_rows, lon), f32)],
        cost_estimate=step_cost,
        name="step",
    )
    final_call = pl.pallas_call(
        final_kernel,
        in_specs=[smem] + [vmem] * 4,
        out_specs=vmem,
        out_shape=jax.ShapeDtypeStruct((comps, rows, lon), f32),
        scratch_shapes=[pltpu.VMEM((comps, near_rows, lon), f32)],
        cost_estimate=step_cost,
        name="final",
    )

    own = increments[0]
    edge = jnp.concatenate([own[:, :FAR], own[:, rows - FAR :]], 1)
    inner = own[:, FAR : rows - FAR]
    costs = []
    for turn in range(ITERS):
        away = turn % 2 == 0
        target = (me ^ 1) if away else me
        shift = inward if away else outward
        mid_e = lax.ppermute(edge, "tm", swap)
        far_e = lax.ppermute(edge, "tm", shift)
        mid_m = lax.ppermute(inner, "tm", swap)
        far_m = lax.ppermute(inner, "tm", shift)
        words, scale, value = other_list if away else own_list
        obs_a, obs_b = deposited(words.astype(jnp.int32), scale, value)
        from_north = lax.ppermute(
            jnp.concatenate(
                [edge[:, 2 * FAR - NEAR :], mid_e[:, FAR:], far_e[:, 2 * FAR - NEAR :]], 1
            ),
            "space",
            southward,
        )
        from_south = lax.ppermute(
            jnp.concatenate([edge[:, :NEAR], mid_e[:, :FAR], far_e[:, :NEAR]], 1),
            "space",
            northward,
        )
        own_lo = (even if away else ~even).astype(jnp.int32).reshape(1)
        flags = jnp.stack(
            [band > 0, band < bands - 1, target < windows - 1, target == 0]
        ).astype(f32)
        lam, part, cost = gap_call(
            own_lo,
            flags,
            edge,
            inner,
            mid_e,
            mid_m,
            far_e,
            far_m,
            from_north,
            from_south,
            start_state,
            depth_wide,
            rate_wide,
            weight_wide,
            obs_a,
            obs_b,
        )
        cost = jnp.sum(cost)
        costs.append(lax.ppermute(cost, "tm", swap) if away else cost)
        if turn < ITERS - 1:
            edge, inner = step_call(flags, lam, part, depth_wide, rate_wide)
        else:
            state = final_call(flags, lam, part, depth_wide, rate_wide)
    sums = (jnp.stack(costs) + own_const).reshape(1, ITERS)
    sums = jnp.pad(sums, ((0, 0), (0, LANE - ITERS)))
    spread = sums
    for turn in range(1, bands):
        ring = [(i, (i + turn) % bands) for i in range(bands)]
        spread = spread + lax.ppermute(sums, "space", ring)
    cells = comps * total_rows * lon
    return state[None], (0.5 / cells) * spread[0, :ITERS, None]


def solution(mesh):
    placed = (
        P("tm", None, "space", None),
        P(None, "space", None),
        P("space", None),
        P(None, "space", None),
        P("tm", None),
        P("tm"),
        P("tm", None),
        P("tm", None),
    )
    return jax.shard_map(
        per_device,
        mesh=mesh,
        in_specs=placed,
        out_specs=(P("tm", None, "space", None), P(None, "tm")),
        check_vma=False,
    )
```

```python
import math

import jax
import jax.numpy as jnp
from jax import lax
from jax.experimental import pallas as pl
from jax.experimental.pallas import tpu as pltpu
from jax.sharding import PartitionSpec as P

STEPS = 6
ITERS = 2
COURANT = 0.35
CORIOLIS_MAX = 0.2
STEP_SIZE = 0.2

SUB = 8
LANE = 128
NEAR = 2 * STEPS
FAR = 4 * STEPS
GROUPS = 4
HALF = 0.5 * COURANT
LEAD = 24


def turned(x):
    return pltpu.roll(x, LANE - 1, 1), pltpu.roll(x, 1, 1)


def raw_lon(pair, first, last):
    ahead, behind = pair
    size = ahead.shape[0]
    ahead = jnp.where(last, pltpu.roll(ahead, size - 1, 0), ahead)
    behind = jnp.where(first, pltpu.roll(behind, 1, 0), behind)
    return ahead - behind


def sweep(state, depth, rate, off, halo, edge_ref, forward):
    count = rate.shape[0] - 2 * off
    size = state.shape[1] // count
    north, south = halo - 1, count - halo

    def one(_, carry):
        lane = lax.broadcasted_iota(jnp.int32, (size, LANE), 1)
        first, last = lane == 0, lane == LANE - 1
        flows, tops, pairs_a, pairs_b = {}, {}, {}, {}

        def at(r):
            return pl.ds(size * r, size)

        def coef(r):
            return depth[pl.ds(size * (off + r), size), :]

        def rot(r):
            return rate[pl.ds(off + r, 1), :]

        def masked(r, x):
            if r == north:
                return x * edge_ref[0]
            if r == south:
                return x * edge_ref[1]
            return x

        def prepare(r):
            v = state[1, at(r), :]
            flows[r] = coef(r) * v if forward else v

        def lat(values, r):
            return values[min(r + 1, count - 1)] - values[max(r - 1, 0)]

        def open_a(r):
            if forward:
                pairs_a[r] = turned(coef(r) * state[0, at(r), :])
            else:
                mix = state[0, at(r), :] - rot(r) * state[1, at(r), :]
                state[0, at(r), :] = mix
                pairs_a[r] = turned(mix)

        def close_a(r):
            if r + 1 < count:
                prepare(r + 1)
            slope = raw_lon(pairs_a.pop(r), first, last) + lat(flows, r)
            old = state[2, at(r), :]
            tops[r] = masked(r, old - slope if forward else old + slope)
            state[2, at(r), :] = tops[r]
            pairs_b[r] = turned(tops[r])

        def close_b(r):
            u, v = state[0, at(r), :], state[1, at(r), :]
            slope = raw_lon(pairs_b.pop(r), first, last)
            if r + 1 < count:
                above = state[2, at(r + 1), :]
            else:
                above = tops[r]
            rise = above - state[2, at(max(r - 1, 0)), :]
            if forward:
                u = u + rot(r) * v - slope
                state[0, at(r), :] = u
                state[1, at(r), :] = v - rot(r) * u - rise
            else:
                state[0, at(r), :] = u + coef(r) * slope
                state[1, at(r), :] = v + rot(r) * u + coef(r) * rise

        prepare(0)
        for r in range(-LEAD, count + LEAD):
            if 0 <= r + LEAD < count:
                open_a(r + LEAD)
            if 0 <= r < count:
                close_a(r)
            if 0 <= r - LEAD < count:
                close_b(r - LEAD)
        return carry

    lax.fori_loop(0, STEPS, one, 0)


def over(count, block, body):
    def step(n, carry):
        body(pl.multiple_of(n * block, SUB))
        return carry

    lax.fori_loop(0, count // block, step, 0)


def gap_kernel(
    own_lo,
    flags,
    own_e,
    own_m,
    mid_e,
    mid_m,
    far_e,
    far_m,
    from_north,
    from_south,
    start,
    depth,
    rate,
    weight,
    obs_a,
    obs_b,
    lam_out,
    part_out,
    cost_out,
    lo,
    mid,
    kept,
    hi,
    depth_v,
    rate_v,
    weight_v,
    a_v,
    b_v,
    sems,
):
    size = depth_v.shape[0] // rate_v.shape[0]
    near, far = NEAR * size, FAR * size
    band = kept.shape[1]
    inner = band - 2 * far

    def assemble(dst, halo, e, m, at, slot):
        pieces = [
            (from_north.at[:, pl.ds(at, halo), :], 0, halo),
            (e.at[:, pl.ds(0, far), :], halo, far),
            (m, halo + far, inner),
            (e.at[:, pl.ds(far, far), :], halo + far + inner, far),
            (from_south.at[:, pl.ds(at, halo), :], halo + band, halo),
        ]
        return [
            pltpu.make_async_copy(src, dst.at[:, pl.ds(where, length), :], sems.at[slot + n])
            for n, (src, where, length) in enumerate(pieces)
        ]

    own_at, mid_at, far_at = 0, near, near + far
    is_own_lo = own_lo[0] == 1
    c_depth = pltpu.make_async_copy(depth, depth_v, sems.at[0])
    c_rate = pltpu.make_async_copy(rate, rate_v, sems.at[1])
    c_mid = assemble(mid, far, mid_e, mid_m, mid_at, 2)
    lo_own = assemble(lo, near, own_e, own_m, own_at, 7)
    lo_far = assemble(lo, near, far_e, far_m, far_at, 7)
    hi_own = assemble(hi, near, own_e, own_m, own_at, 12)
    hi_far = assemble(hi, near, far_e, far_m, far_at, 12)
    c_kept = [
        pltpu.make_async_copy(
            mid_e.at[:, pl.ds(0, far), :], kept.at[:, pl.ds(0, far), :], sems.at[17]
        ),
        pltpu.make_async_copy(mid_m, kept.at[:, pl.ds(far, inner), :], sems.at[18]),
        pltpu.make_async_copy(
            mid_e.at[:, pl.ds(far, far), :], kept.at[:, pl.ds(far + inner, far), :], sems.at[19]
        ),
    ]
    c_weight = pltpu.make_async_copy(weight, weight_v, sems.at[20])
    c_a = pltpu.make_async_copy(obs_a, a_v, sems.at[21])
    c_b = pltpu.make_async_copy(obs_b, b_v, sems.at[22])
    c_depth.start()
    c_rate.start()
    for c in c_mid:
        c.start()

    @pl.when(is_own_lo)
    def _():
        for c in lo_own + hi_far:
            c.start()

    @pl.when(jnp.logical_not(is_own_lo))
    def _():
        for c in lo_far + hi_own:
            c.start()

    for c in c_kept + [c_weight, c_a, c_b]:
        c.start()

    c_depth.wait()
    c_rate.wait()
    for c in c_mid:
        c.wait()

    block = 8 * size

    def scale_third(ref, where, length):
        def body(n):
            at = pl.ds(where + n, block)
            ref[2, at, :] = ref[2, at, :] * HALF

        over(length, block, body)

    scale_third(mid, 0, mid.shape[1])
    sweep(mid, depth_v, rate_v, 0, FAR, flags, True)
    for c in lo_own:
        c.wait()

    scale_third(lo, 0, lo.shape[1])
    sweep(lo, depth_v, rate_v, FAR - NEAR, NEAR, flags, True)
    for c in hi_own + [c_weight]:
        c.wait()

    for part in range(3):
        back_scale = 1.0 / HALF if part == 2 else 1.0

        def body(n):
            at = pl.ds(n, block)
            end = mid[part, pl.ds(far - near + n, block), :] * back_scale
            lam = weight_v[part, at, :] * (hi[part, at, :] - end)
            lam_out[part, at, :] = lam * (flags[2] * back_scale)

        over(hi.shape[1], block, body)

    for c in c_kept + [c_a, c_b]:
        c.wait()

    @pl.when(flags[3] > 0.5)
    def _():
        c = pltpu.make_async_copy(start, lo.at[:, pl.ds(near, band), :], sems.at[0])
        c.start()
        c.wait()
        scale_third(lo, near, band)

    cost_out[...] = jnp.zeros_like(cost_out)
    for part in range(3):
        back_scale = 1.0 / HALF if part == 2 else 1.0

        def body(n):
            at, shifted = pl.ds(n, block), pl.ds(near + n, block)
            here = kept[part, at, :]
            gap = here - lo[part, shifted, :] * back_scale
            lam = weight_v[part, shifted, :] * gap
            pull = a_v[part, at, :] * here
            part_out[part, at, :] = here - STEP_SIZE * (lam + (pull - b_v[part, at, :]))
            cost_out[...] += lam * gap + here * (pull - 2.0 * b_v[part, at, :])

        over(band, block, body)


def step_kernel(flags, lam, part, depth, rate, edge_out, mid_out, work):
    band = part.shape[1]
    size = depth.shape[0] // rate.shape[0]
    near, far = NEAR * size, FAR * size
    block = 8 * size
    work[...] = lam[...]
    sweep(work, depth, rate, FAR - NEAR, NEAR, flags, False)
    for c in range(3):
        scale = STEP_SIZE * (HALF if c == 2 else 1.0)

        def new(where):
            return part[c, pl.ds(where, block), :] + scale * work[c, pl.ds(near + where, block), :]

        def upper(n):
            edge_out[c, pl.ds(n, block), :] = new(n)
            edge_out[c, pl.ds(far + n, block), :] = new(band - far + n)

        def middle(n):
            mid_out[c, pl.ds(n, block), :] = new(far + n)

        over(far, block, upper)
        over(band - 2 * far, block, middle)


def final_kernel(flags, lam, part, depth, rate, out, work):
    size = depth.shape[0] // rate.shape[0]
    near = NEAR * size
    work[...] = lam[...]
    sweep(work, depth, rate, FAR - NEAR, NEAR, flags, False)
    for c in range(3):
        scale = STEP_SIZE * (HALF if c == 2 else 1.0)

        def body(t, carry):
            base = t * (SUB * size)
            for s in range(size):
                here = part[c, pl.ds(base + s, SUB, stride=size), :]
                back = work[c, pl.ds(near + base + s, SUB, stride=size), :]
                out[c, pl.ds(pl.multiple_of(t * SUB, SUB), SUB), pl.ds(s * LANE, LANE)] = (
                    here + scale * back
                )
            return carry

        lax.fori_loop(0, out.shape[1] // SUB, body, 0)


def deposit_kernel(code, load, value, a_out, b_out, *acc):
    a_acc, b_acc = acc[:GROUPS], acc[GROUPS:]
    size = acc[0].shape[0] - a_out.shape[0]
    block = 8 * size
    zero = jnp.zeros((block, LANE), jnp.float32)

    def clear(n):
        for ref in acc:
            ref[pl.ds(n, block), :] = zero

    over(a_out.shape[0], block, clear)
    column = lax.broadcasted_iota(jnp.int32, (size, LANE), 0) * LANE + lax.broadcasted_iota(
        jnp.int32, (size, LANE), 1
    )
    shift = (size * LANE).bit_length() - 1

    def body(n, carry):
        for g in range(GROUPS):
            i = n * GROUPS + g
            word = code[i]
            at = pl.ds(pl.multiple_of((word >> shift) * size, size), size)
            hit = column == (word & (size * LANE - 1))
            a_acc[g][at, :] = a_acc[g][at, :] + jnp.where(hit, load[i], 0.0)
            b_acc[g][at, :] = b_acc[g][at, :] + jnp.where(hit, value[i], 0.0)
        return carry

    lax.fori_loop(0, code.shape[0] // GROUPS, body, 0, unroll=4)

    def total(n):
        at = pl.ds(n, block)
        for out, refs in ((a_out, a_acc), (b_out, b_acc)):
            out[at, :] = (refs[0][at, :] + refs[1][at, :]) + (refs[2][at, :] + refs[3][at, :])

    over(a_out.shape[0], block, total)


def per_device(
    increments, start_state, depth, error_weight, obs_index, obs_count, obs_value, obs_weight
):
    _, comps, rows, lon = increments.shape
    bands = lax.axis_size("space")
    windows = lax.axis_size("tm")
    band = lax.axis_index("space")
    me = lax.axis_index("tm")
    even = me % 2 == 0
    total_rows = rows * bands
    first_row = band * rows
    size = lon // LANE
    f32 = jnp.float32
    any_space = pl.BlockSpec(memory_space=pl.ANY)
    smem = pl.BlockSpec(memory_space=pltpu.SMEM)
    vmem = pl.BlockSpec(memory_space=pltpu.VMEM)

    def folded(x):
        return x.reshape(x.shape[:-2] + (x.shape[-2] * size, LANE))

    swap = [(i, i ^ 1) for i in range(windows)]
    inward = [(i, i - 2) for i in range(2, windows) if i % 2 == 0] + [
        (i, i + 2) for i in range(windows - 2) if i % 2 == 1
    ]
    outward = [(b, a) for a, b in inward]
    southward = [(i, i + 1) for i in range(bands - 1)]
    northward = [(b, a) for a, b in southward]
    near, far = NEAR * size, FAR * size
    band_size = rows * size

    own = folded(increments[0])
    edge = jnp.concatenate([own[:, :far], own[:, band_size - far :]], 1)
    inner = own[:, far : band_size - far]

    index = obs_index[0]
    plane = total_rows * lon
    component = index // plane
    remainder = index % plane
    local = remainder // lon - first_row
    kept = (local >= 0) & (local < rows) & (jnp.arange(index.shape[0]) < obs_count[0])
    code = jnp.where(kept, (component * rows + local) * lon + remainder % lon, comps * rows * lon)
    load = jnp.where(kept, obs_weight[0], 0.0)
    pulled = load * obs_value[0]
    own_list = jnp.stack([code.astype(f32), load, pulled])
    own_const = jnp.sum(pulled * obs_value[0])
    other_list = lax.ppermute(own_list, "tm", swap)

    deposit = pl.pallas_call(
        deposit_kernel,
        in_specs=[smem] * 3,
        out_specs=[vmem] * 2,
        out_shape=[jax.ShapeDtypeStruct((comps * band_size, LANE), f32)] * 2,
        scratch_shapes=[pltpu.VMEM((comps * band_size + size, LANE), f32)] * (2 * GROUPS),
        cost_estimate=pl.CostEstimate(flops=40_000_000, bytes_accessed=0, transcendentals=0),
        name="deposit",
    )

    def deposited(words):
        a, b = deposit(words[0].astype(jnp.int32), words[1], words[2])
        return a.reshape(comps, band_size, LANE), b.reshape(comps, band_size, LANE)

    const = jnp.concatenate([folded(error_weight).reshape(-1, LANE), folded(depth)], 0)
    pieces = [const[c * band_size : (c + 1) * band_size] for c in range(comps + 1)]
    sizes = [near] * comps + [far]
    const_n = lax.ppermute(
        jnp.concatenate([p[band_size - n :] for p, n in zip(pieces, sizes)]), "space", southward
    )
    const_s = lax.ppermute(
        jnp.concatenate([p[:n] for p, n in zip(pieces, sizes)]), "space", northward
    )
    split = comps * near
    shaped = lambda c: c[:split].reshape(comps, near, LANE)
    weight_wide = jnp.concatenate([shaped(const_n), folded(error_weight), shaped(const_s)], 1)
    depth_wide = (HALF * HALF) * jnp.concatenate([const_n[split:], pieces[-1], const_s[split:]], 0)
    latitude = (
        (first_row - FAR + jnp.arange(rows + 2 * FAR)).astype(f32) + 0.5
    ) / total_rows * math.pi - math.pi / 2
    rate_wide = jnp.broadcast_to(
        (CORIOLIS_MAX * jnp.sin(latitude))[:, None], (rows + 2 * FAR, LANE)
    )
    start = folded(start_state)

    near_size, far_size = band_size + 2 * near, band_size + 2 * far
    gap_call = pl.pallas_call(
        gap_kernel,
        in_specs=[smem, smem] + [any_space] * 14,
        out_specs=[vmem] * 3,
        out_shape=[
            jax.ShapeDtypeStruct((comps, near_size, LANE), f32),
            jax.ShapeDtypeStruct((comps, band_size, LANE), f32),
            jax.ShapeDtypeStruct((8 * size, LANE), f32),
        ],
        scratch_shapes=[
            pltpu.VMEM((comps, near_size, LANE), f32),
            pltpu.VMEM((comps, far_size, LANE), f32),
            pltpu.VMEM((comps, band_size, LANE), f32),
            pltpu.VMEM((comps, near_size, LANE), f32),
            pltpu.VMEM((far_size, LANE), f32),
            pltpu.VMEM((rows + 2 * FAR, LANE), f32),
            pltpu.VMEM((comps, near_size, LANE), f32),
            pltpu.VMEM((comps, band_size, LANE), f32),
            pltpu.VMEM((comps, band_size, LANE), f32),
            pltpu.SemaphoreType.DMA((23,)),
        ],
        cost_estimate=pl.CostEstimate(flops=30_000_000, bytes_accessed=0, transcendentals=0),
        name="gaps",
    )
    step_cost = pl.CostEstimate(flops=15_000_000, bytes_accessed=0, transcendentals=0)
    step_call = pl.pallas_call(
        step_kernel,
        in_specs=[smem] + [vmem] * 4,
        out_specs=[vmem] * 2,
        out_shape=[
            jax.ShapeDtypeStruct((comps, 2 * far, LANE), f32),
            jax.ShapeDtypeStruct((comps, band_size - 2 * far, LANE), f32),
        ],
        scratch_shapes=[pltpu.VMEM((comps, near_size, LANE), f32)],
        cost_estimate=step_cost,
        name="step",
    )
    final_call = pl.pallas_call(
        final_kernel,
        in_specs=[smem] + [vmem] * 4,
        out_specs=vmem,
        out_shape=jax.ShapeDtypeStruct((comps, rows, lon), f32),
        scratch_shapes=[pltpu.VMEM((comps, near_size, LANE), f32)],
        cost_estimate=step_cost,
        name="final",
    )

    costs = []
    own_obs = deposited(own_list)
    for turn in range(ITERS):
        away = turn % 2 == 0
        target = (me ^ 1) if away else me
        shift = inward if away else outward
        mid_e = lax.ppermute(edge, "tm", swap)
        far_e = lax.ppermute(edge, "tm", shift)
        mid_m = lax.ppermute(inner, "tm", swap)
        far_m = lax.ppermute(inner, "tm", shift)
        if turn == 0:
            own_obs, mid_e, other_list = lax.optimization_barrier((own_obs, mid_e, other_list))
            other_obs = deposited(other_list)
        obs_a, obs_b = other_obs if away else own_obs
        from_north = lax.ppermute(
            jnp.concatenate(
                [edge[:, 2 * far - near :], mid_e[:, far:], far_e[:, 2 * far - near :]], 1
            ),
            "space",
            southward,
        )
        from_south = lax.ppermute(
            jnp.concatenate([edge[:, :near], mid_e[:, :far], far_e[:, :near]], 1),
            "space",
            northward,
        )
        own_lo = (even if away else ~even).astype(jnp.int32).reshape(1)
        flags = jnp.stack(
            [band > 0, band < bands - 1, target < windows - 1, target == 0]
        ).astype(f32)
        lam, part, cost = gap_call(
            own_lo,
            flags,
            edge,
            inner,
            mid_e,
            mid_m,
            far_e,
            far_m,
            from_north,
            from_south,
            start,
            depth_wide,
            rate_wide,
            weight_wide,
            obs_a,
            obs_b,
        )
        cost = jnp.sum(cost)
        costs.append(lax.ppermute(cost, "tm", swap) if away else cost)
        if turn < ITERS - 1:
            edge, inner = step_call(flags, lam, part, depth_wide, rate_wide)
        else:
            state = final_call(flags, lam, part, depth_wide, rate_wide)
    sums = (jnp.stack(costs) + own_const).reshape(1, ITERS)
    sums = jnp.pad(sums, ((0, 0), (0, LANE - ITERS)))
    spread = sums
    for turn in range(1, bands):
        ring = [(i, (i + turn) % bands) for i in range(bands)]
        spread = spread + lax.ppermute(sums, "space", ring)
    cells = comps * total_rows * lon
    return state[None], (0.5 / cells) * spread[0, :ITERS, None]


def solution(mesh):
    placed = (
        P("tm", None, "space", None),
        P(None, "space", None),
        P("space", None),
        P(None, "space", None),
        P("tm", None),
        P("tm"),
        P("tm", None),
        P("tm", None),
    )
    return jax.shard_map(
        per_device,
        mesh=mesh,
        in_specs=placed,
        out_specs=(P("tm", None, "space", None), P(None, "tm")),
        check_vma=False,
    )
```

```python
import functools
import math

import jax
import jax.numpy as jnp
from jax import lax
from jax.experimental import pallas as pl
from jax.experimental.pallas import tpu as pltpu
from jax.sharding import PartitionSpec as P


STEPS = 6
ITERS = 2
COURANT = 0.35
CORIOLIS_MAX = 0.2
STEP_SIZE = 0.2

SUB = 8
LANE = 128
NEAR = 2 * STEPS
FAR = 4 * STEPS
GROUPS = 4
DEALS = 4
HALF = 0.5 * COURANT
LEAD = 24


def turned(x):
    return pltpu.roll(x, LANE - 1, 1), pltpu.roll(x, 1, 1)


def raw_lon(pair, first, last):
    ahead, behind = pair
    size = ahead.shape[0]
    ahead = jnp.where(last, pltpu.roll(ahead, size - 1, 0), ahead)
    behind = jnp.where(first, pltpu.roll(behind, 1, 0), behind)
    return ahead - behind


def sweep(state, depth, rate, off, halo, edge_ref, forward):
    count = rate.shape[0] - 2 * off
    size = state.shape[1] // count
    north, south = halo - 1, count - halo

    def one(_, carry):
        lane = lax.broadcasted_iota(jnp.int32, (size, LANE), 1)
        first, last = lane == 0, lane == LANE - 1
        flows, tops, pairs_a, pairs_b = {}, {}, {}, {}

        def at(r):
            return pl.ds(size * r, size)

        def coef(r):
            return depth[pl.ds(size * (off + r), size), :]

        def rot(r):
            return rate[pl.ds(off + r, 1), :]

        def masked(r, x):
            if r == north:
                return x * edge_ref[0]
            if r == south:
                return x * edge_ref[1]
            return x

        def prepare(r):
            v = state[1, at(r), :]
            flows[r] = coef(r) * v if forward else v

        def lat(values, r):
            return values[min(r + 1, count - 1)] - values[max(r - 1, 0)]

        def open_a(r):
            if forward:
                pairs_a[r] = turned(coef(r) * state[0, at(r), :])
            else:
                mix = state[0, at(r), :] - rot(r) * state[1, at(r), :]
                state[0, at(r), :] = mix
                pairs_a[r] = turned(mix)

        def close_a(r):
            if r + 1 < count:
                prepare(r + 1)
            slope = raw_lon(pairs_a.pop(r), first, last) + lat(flows, r)
            old = state[2, at(r), :]
            tops[r] = masked(r, old - slope if forward else old + slope)
            state[2, at(r), :] = tops[r]
            pairs_b[r] = turned(tops[r])

        def close_b(r):
            u, v = state[0, at(r), :], state[1, at(r), :]
            slope = raw_lon(pairs_b.pop(r), first, last)
            if r + 1 < count:
                above = state[2, at(r + 1), :]
            else:
                above = tops[r]
            rise = above - state[2, at(max(r - 1, 0)), :]
            if forward:
                u = u + rot(r) * v - slope
                state[0, at(r), :] = u
                state[1, at(r), :] = v - rot(r) * u - rise
            else:
                state[0, at(r), :] = u + coef(r) * slope
                state[1, at(r), :] = v + rot(r) * u + coef(r) * rise

        prepare(0)
        for r in range(-LEAD, count + LEAD):
            if 0 <= r + LEAD < count:
                open_a(r + LEAD)
            if 0 <= r < count:
                close_a(r)
            if 0 <= r - LEAD < count:
                close_b(r - LEAD)
        return carry

    lax.fori_loop(0, STEPS, one, 0)


def over(count, block, body):
    def step(n, carry):
        body(pl.multiple_of(n * block, SUB))
        return carry

    trips = count // block
    lax.fori_loop(0, trips, step, 0, unroll=2 if trips % 2 == 0 else 1)


def round_kernel(
    finish,
    own_lo,
    flags,
    own_e,
    own_m,
    mid_e,
    mid_m,
    far_e,
    far_m,
    from_north,
    from_south,
    start,
    depth,
    rate,
    weight,
    obs_a,
    obs_b,
    *refs,
):
    outs, cost_out = refs[:finish], refs[finish]
    lo, mid, kept, hi, depth_v, rate_v, weight_v, a_v, b_v, cost_v, sems = refs[finish + 1 :]
    size = depth_v.shape[0] // rate_v.shape[0]
    near, far = NEAR * size, FAR * size
    band = kept.shape[1]
    inner = band - 2 * far

    def assemble(dst, halo, e, m, at, slot):
        pieces = [
            (from_north.at[:, pl.ds(at, halo), :], 0, halo),
            (e.at[:, pl.ds(0, far), :], halo, far),
            (m, halo + far, inner),
            (e.at[:, pl.ds(far, far), :], halo + far + inner, far),
            (from_south.at[:, pl.ds(at, halo), :], halo + band, halo),
        ]
        return [
            pltpu.make_async_copy(src, dst.at[:, pl.ds(where, length), :], sems.at[slot + n])
            for n, (src, where, length) in enumerate(pieces)
        ]

    own_at, mid_at, far_at = 0, near, near + far
    is_own_lo = own_lo[0] == 1
    c_depth = pltpu.make_async_copy(depth, depth_v, sems.at[0])
    c_rate = pltpu.make_async_copy(rate, rate_v, sems.at[1])
    c_mid = assemble(mid, far, mid_e, mid_m, mid_at, 2)
    lo_own = assemble(lo, near, own_e, own_m, own_at, 7)
    lo_far = assemble(lo, near, far_e, far_m, far_at, 7)
    hi_own = assemble(hi, near, own_e, own_m, own_at, 12)
    hi_far = assemble(hi, near, far_e, far_m, far_at, 12)
    c_kept = [
        pltpu.make_async_copy(
            mid_e.at[:, pl.ds(0, far), :], kept.at[:, pl.ds(0, far), :], sems.at[17]
        ),
        pltpu.make_async_copy(mid_m, kept.at[:, pl.ds(far, inner), :], sems.at[18]),
        pltpu.make_async_copy(
            mid_e.at[:, pl.ds(far, far), :], kept.at[:, pl.ds(far + inner, far), :], sems.at[19]
        ),
    ]
    c_weight = pltpu.make_async_copy(weight, weight_v, sems.at[20])
    c_a = pltpu.make_async_copy(obs_a, a_v, sems.at[21])
    c_b = pltpu.make_async_copy(obs_b, b_v, sems.at[22])
    c_depth.start()
    c_rate.start()
    for c in c_mid:
        c.start()

    @pl.when(is_own_lo)
    def _():
        for c in lo_own + hi_far:
            c.start()

    @pl.when(jnp.logical_not(is_own_lo))
    def _():
        for c in lo_far + hi_own:
            c.start()

    for c in c_kept + [c_weight, c_a, c_b]:
        c.start()

    c_depth.wait()
    c_rate.wait()
    for c in c_mid:
        c.wait()

    block = 8 * size

    def scale_third(ref, where, length):
        def body(n):
            at = pl.ds(where + n, block)
            ref[2, at, :] = ref[2, at, :] * HALF

        over(length, block, body)

    scale_third(mid, 0, mid.shape[1])
    sweep(mid, depth_v, rate_v, 0, FAR, flags, True)
    for c in lo_own:
        c.wait()

    scale_third(lo, 0, lo.shape[1])
    sweep(lo, depth_v, rate_v, FAR - NEAR, NEAR, flags, True)
    for c in hi_own + [c_weight]:
        c.wait()

    for part in range(3):
        back_scale = 1.0 / HALF if part == 2 else 1.0

        def body(n):
            at = pl.ds(n, block)
            end = mid[part, pl.ds(far - near + n, block), :] * back_scale
            lam = weight_v[part, at, :] * (hi[part, at, :] - end)
            hi[part, at, :] = lam * (flags[2] * back_scale)

        over(hi.shape[1], block, body)

    for c in c_kept + [c_a, c_b]:
        c.wait()

    @pl.when(flags[3] > 0.5)
    def _():
        c = pltpu.make_async_copy(start, lo.at[:, pl.ds(near, band), :], sems.at[0])
        c.start()
        c.wait()
        scale_third(lo, near, band)

    cost_v[...] = jnp.zeros_like(cost_v)
    for part in range(3):
        back_scale = 1.0 / HALF if part == 2 else 1.0

        def body(n):
            at, shifted = pl.ds(n, block), pl.ds(near + n, block)
            here = kept[part, at, :]
            gap = here - lo[part, shifted, :] * back_scale
            lam = weight_v[part, shifted, :] * gap
            pull = a_v[part, at, :] * here
            kept[part, at, :] = here - STEP_SIZE * (lam + (pull - b_v[part, at, :]))
            cost_v[...] += lam * gap + here * (pull - 2.0 * b_v[part, at, :])

        over(band, block, body)

    total = cost_v[pl.ds(0, SUB), :]
    for n in range(1, cost_v.shape[0] // SUB):
        total = total + cost_v[pl.ds(SUB * n, SUB), :]
    cost_out[...] = total

    sweep(hi, depth_v, rate_v, FAR - NEAR, NEAR, flags, False)
    for part in range(3):
        scale = STEP_SIZE * (HALF if part == 2 else 1.0)

        def new(where):
            return kept[part, pl.ds(where, block), :] + scale * hi[part, pl.ds(near + where, block), :]

        def upper(n):
            outs[0][part, pl.ds(n, block), :] = new(n)
            outs[0][part, pl.ds(far + n, block), :] = new(band - far + n)

        def middle(n):
            outs[1][part, pl.ds(n, block), :] = new(far + n)

        def last(t, carry):
            base = t * (SUB * size)
            for s in range(size):
                here = kept[part, pl.ds(base + s, SUB, stride=size), :]
                back = hi[part, pl.ds(near + base + s, SUB, stride=size), :]
                at = pl.ds(pl.multiple_of(t * SUB, SUB), SUB)
                outs[0][part, at, pl.ds(s * LANE, LANE)] = here + scale * back
            return carry

        if finish == 2:
            over(far, block, upper)
            over(inner, block, middle)
        else:
            lax.fori_loop(0, outs[0].shape[1] // SUB, last, 0)


def deposit_kernel(code, load, value, a_out, b_out, picked, *acc):
    a_acc, b_acc = acc[:GROUPS], acc[GROUPS:]
    size = acc[0].shape[0] - a_out.shape[0]
    block = 8 * size
    zero = jnp.zeros((block, LANE), jnp.float32)

    def clear(n):
        for ref in acc:
            ref[pl.ds(n, block), :] = zero

    over(a_out.shape[0], block, clear)
    column = lax.broadcasted_iota(jnp.int32, (size, LANE), 0) * LANE + lax.broadcasted_iota(
        jnp.int32, (size, LANE), 1
    )
    shift = (size * LANE).bit_length() - 1
    spare = (a_out.shape[0] // size) << shift
    entries = code.shape[0] - GROUPS * DEALS

    def pick(n, found):
        for k in range(GROUPS * DEALS):
            i = n * (GROUPS * DEALS) + k
            picked[found] = i
            found = found + (code[i] < spare).astype(jnp.int32)
        return found

    found = lax.fori_loop(0, entries // (GROUPS * DEALS), pick, 0)
    for k in range(GROUPS * DEALS):
        picked[found + k] = entries

    def body(n, carry):
        for k in range(DEALS):
            for g in range(GROUPS):
                i = picked[n * (GROUPS * DEALS) + (k * GROUPS + g)]
                word = code[i]
                at = pl.ds(pl.multiple_of((word >> shift) * size, size), size)
                hit = column == (word & (size * LANE - 1))
                a_acc[g][at, :] = a_acc[g][at, :] + jnp.where(hit, load[i], 0.0)
                b_acc[g][at, :] = b_acc[g][at, :] + jnp.where(hit, value[i], 0.0)
        return carry

    lax.fori_loop(0, (found + GROUPS * DEALS - 1) // (GROUPS * DEALS), body, 0)

    def total(n):
        at = pl.ds(n, block)
        for out, refs in ((a_out, a_acc), (b_out, b_acc)):
            out[at, :] = (refs[0][at, :] + refs[1][at, :]) + (refs[2][at, :] + refs[3][at, :])

    over(a_out.shape[0], block, total)


def per_device(
    increments, start_state, depth, error_weight, obs_index, obs_count, obs_value, obs_weight
):
    _, comps, rows, lon = increments.shape
    bands = lax.axis_size("space")
    windows = lax.axis_size("tm")
    band = lax.axis_index("space")
    me = lax.axis_index("tm")
    even = me % 2 == 0
    total_rows = rows * bands
    first_row = band * rows
    size = lon // LANE
    f32 = jnp.float32
    any_space = pl.BlockSpec(memory_space=pl.ANY)
    smem = pl.BlockSpec(memory_space=pltpu.SMEM)
    vmem = pl.BlockSpec(memory_space=pltpu.VMEM)

    def folded(x):
        return x.reshape(x.shape[:-2] + (x.shape[-2] * size, LANE))

    swap = [(i, i ^ 1) for i in range(windows)]
    inward = [(i, i - 2) for i in range(2, windows) if i % 2 == 0] + [
        (i, i + 2) for i in range(windows - 2) if i % 2 == 1
    ]
    outward = [(b, a) for a, b in inward]
    southward = [(i, i + 1) for i in range(bands - 1)]
    northward = [(b, a) for a, b in southward]
    near, far = NEAR * size, FAR * size
    band_size = rows * size

    own = folded(increments[0])
    edge = jnp.concatenate([own[:, :far], own[:, band_size - far :]], 1)
    inner = own[:, far : band_size - far]

    index = obs_index[0]
    plane = total_rows * lon
    component = index // plane
    remainder = index % plane
    local = remainder // lon - first_row
    kept = (local >= 0) & (local < rows) & (jnp.arange(index.shape[0]) < obs_count[0])
    code = jnp.where(kept, (component * rows + local) * lon + remainder % lon, comps * rows * lon)
    load = jnp.where(kept, obs_weight[0], 0.0)
    pulled = load * obs_value[0]
    own_list = jnp.stack([code.astype(f32), load, pulled])
    own_const = jnp.sum(pulled * obs_value[0])
    other_list = lax.ppermute(own_list, "tm", swap)

    def kernel(body, in_specs, out_specs, outs, scratch, flops):
        held = sum(math.prod(o.shape) for o in outs)
        held += sum(math.prod(c.shape) for c in scratch if c.dtype == f32)
        return pl.pallas_call(
            body,
            in_specs=in_specs,
            out_specs=out_specs,
            out_shape=outs,
            scratch_shapes=scratch,
            cost_estimate=pl.CostEstimate(flops=flops, bytes_accessed=0, transcendentals=0),
            compiler_params=pltpu.CompilerParams(vmem_limit_bytes=4 * held + (4 << 20)),
        )

    extra = GROUPS * DEALS
    deposit = kernel(
        deposit_kernel,
        [smem] * 3,
        [vmem] * 2,
        [jax.ShapeDtypeStruct((comps * band_size, LANE), f32)] * 2,
        [pltpu.SMEM((index.shape[0] + extra,), jnp.int32)]
        + [pltpu.VMEM((comps * band_size + size, LANE), f32)] * (2 * GROUPS),
        20_000_000,
    )

    def deposited(words):
        spare = jnp.full((extra,), comps * rows * lon, jnp.int32)
        none = jnp.zeros((extra,), f32)
        a, b = deposit(
            jnp.concatenate([words[0].astype(jnp.int32), spare]),
            jnp.concatenate([words[1], none]),
            jnp.concatenate([words[2], none]),
        )
        return a.reshape(comps, band_size, LANE), b.reshape(comps, band_size, LANE)

    const = jnp.concatenate([folded(error_weight).reshape(-1, LANE), folded(depth)], 0)
    pieces = [const[c * band_size : (c + 1) * band_size] for c in range(comps + 1)]
    sizes = [near] * comps + [far]
    const_n = lax.ppermute(
        jnp.concatenate([p[band_size - n :] for p, n in zip(pieces, sizes)]),
        "space",
        southward,
    )
    const_s = lax.ppermute(
        jnp.concatenate([p[:n] for p, n in zip(pieces, sizes)]), "space", northward
    )
    split = comps * near
    shaped = lambda c: c[:split].reshape(comps, near, LANE)
    weight_wide = jnp.concatenate([shaped(const_n), folded(error_weight), shaped(const_s)], 1)
    depth_wide = (HALF * HALF) * jnp.concatenate([const_n[split:], pieces[-1], const_s[split:]], 0)
    latitude = (
        (first_row - FAR + jnp.arange(rows + 2 * FAR)).astype(f32) + 0.5
    ) / total_rows * math.pi - math.pi / 2
    rate_wide = jnp.broadcast_to(
        (CORIOLIS_MAX * jnp.sin(latitude))[:, None], (rows + 2 * FAR, LANE)
    )
    start = folded(start_state)

    near_size, far_size = band_size + 2 * near, band_size + 2 * far
    tile = jax.ShapeDtypeStruct((SUB, LANE), f32)

    def round_call(finish, outs):
        return kernel(
            functools.partial(round_kernel, finish),
            [smem, smem] + [any_space] * 14,
            [vmem] * (finish + 1),
            outs + [tile],
            [
                pltpu.VMEM((comps, near_size, LANE), f32),
                pltpu.VMEM((comps, far_size, LANE), f32),
                pltpu.VMEM((comps, band_size, LANE), f32),
                pltpu.VMEM((comps, near_size, LANE), f32),
                pltpu.VMEM((far_size, LANE), f32),
                pltpu.VMEM((rows + 2 * FAR, LANE), f32),
                pltpu.VMEM((comps, near_size, LANE), f32),
                pltpu.VMEM((comps, band_size, LANE), f32),
                pltpu.VMEM((comps, band_size, LANE), f32),
                pltpu.VMEM((8 * size, LANE), f32),
                pltpu.SemaphoreType.DMA((23,)),
            ],
            45_000_000,
        )

    def ring_sum(x):
        total = x
        for turn in range(1, bands):
            ring = [(i, (i + turn) % bands) for i in range(bands)]
            total = total + lax.ppermute(x, "space", ring)
        return total

    for turn in range(ITERS):
        away = turn % 2 == 0
        target = (me ^ 1) if away else me
        shift = inward if away else outward
        mid_e = lax.ppermute(edge, "tm", swap)
        far_e = lax.ppermute(edge, "tm", shift)
        mid_m = lax.ppermute(inner, "tm", swap)
        far_m = lax.ppermute(inner, "tm", shift)
        obs_a, obs_b = deposited(other_list if away else own_list)
        from_north = lax.ppermute(
            jnp.concatenate(
                [edge[:, 2 * far - near :], mid_e[:, far:], far_e[:, 2 * far - near :]], 1
            ),
            "space",
            southward,
        )
        from_south = lax.ppermute(
            jnp.concatenate([edge[:, :near], mid_e[:, :far], far_e[:, :near]], 1),
            "space",
            northward,
        )
        own_lo = (even if away else ~even).astype(jnp.int32).reshape(1)
        flags = jnp.stack(
            [band > 0, band < bands - 1, target < windows - 1, target == 0]
        ).astype(f32)
        if turn < ITERS - 1:
            outs = [
                jax.ShapeDtypeStruct((comps, 2 * far, LANE), f32),
                jax.ShapeDtypeStruct((comps, band_size - 2 * far, LANE), f32),
            ]
        else:
            outs = [jax.ShapeDtypeStruct((comps, rows, lon), f32)]
        *state, cost = round_call(len(outs), outs)(
            own_lo,
            flags,
            edge,
            inner,
            mid_e,
            mid_m,
            far_e,
            far_m,
            from_north,
            from_south,
            start,
            depth_wide,
            rate_wide,
            weight_wide,
            obs_a,
            obs_b,
        )
        if turn == 0:
            edge, inner = state
            edge, own_list = lax.optimization_barrier((edge, own_list))
            cost = lax.ppermute(cost, "tm", swap)
            fixed = jnp.full((SUB, LANE), own_const / (SUB * LANE))
            early = ring_sum(jnp.stack([cost + fixed, fixed]))
    cells = comps * total_rows * lon
    late = ring_sum(cost) + early[1]
    costs = (0.5 / cells) * jnp.stack([jnp.sum(early[0]), jnp.sum(late)])
    return state[0][None], costs[:, None]


def solution(mesh):
    placed = (
        P("tm", None, "space", None),
        P(None, "space", None),
        P("space", None),
        P(None, "space", None),
        P("tm", None),
        P("tm"),
        P("tm", None),
        P("tm", None),
    )

    return jax.shard_map(
        per_device,
        mesh=mesh,
        in_specs=placed,
        out_specs=(P("tm", None, "space", None), P(None, "tm")),
        check_vma=False,
    )
```

```python
import functools
import math

import jax
import jax.numpy as jnp
from jax import lax
from jax.experimental import pallas as pl
from jax.experimental.pallas import tpu as pltpu
from jax.sharding import PartitionSpec as P


STEPS = 6
ITERS = 2
COURANT = 0.35
CORIOLIS_MAX = 0.2
STEP_SIZE = 0.2

SUB = 8
LANE = 128
NEAR = 2 * STEPS
FAR = 4 * STEPS
GROUPS = 4
DEALS = 4
HALF = 0.5 * COURANT
LEAD = 24

EDGE_W = 16


def turned(x):
    return pltpu.roll(x, LANE - 1, 1), pltpu.roll(x, 1, 1)


def raw_lon(pair, first, last):
    ahead, behind = pair
    size = ahead.shape[0]
    ahead = jnp.where(last, pltpu.roll(ahead, size - 1, 0), ahead)
    behind = jnp.where(first, pltpu.roll(behind, 1, 0), behind)
    return ahead - behind


def sweep(state, depth, rate, off, halo, edge_ref, forward):
    count = rate.shape[0] - 2 * off
    north, south = halo - 1, count - halo

    def one(_, carry):
        lane = lax.broadcasted_iota(jnp.int32, depth.shape[1:], 1)
        first, last = lane == 0, lane == LANE - 1
        flows, tops, pairs_a, pairs_b = {}, {}, {}, {}

        def coef(r):
            return depth[off + r]

        def rot(r):
            return rate[pl.ds(off + r, 1), :]

        def masked(r, x):
            if r == north:
                return x * edge_ref[0]
            if r == south:
                return x * edge_ref[1]
            return x

        def prepare(r):
            v = state[1, r]
            flows[r] = coef(r) * v if forward else v

        def lat(values, r):
            return values[min(r + 1, count - 1)] - values[max(r - 1, 0)]

        def open_a(r):
            if forward:
                pairs_a[r] = turned(coef(r) * state[0, r])
            else:
                mix = state[0, r] - rot(r) * state[1, r]
                state[0, r] = mix
                pairs_a[r] = turned(mix)

        def close_a(r):
            if r + 1 < count:
                prepare(r + 1)
            slope = raw_lon(pairs_a.pop(r), first, last) + lat(flows, r)
            old = state[2, r]
            tops[r] = masked(r, old - slope if forward else old + slope)
            state[2, r] = tops[r]
            pairs_b[r] = turned(tops[r])

        def close_b(r):
            u, v = state[0, r], state[1, r]
            slope = raw_lon(pairs_b.pop(r), first, last)
            if r + 1 < count:
                above = state[2, r + 1]
            else:
                above = tops[r]
            rise = above - state[2, max(r - 1, 0)]
            if forward:
                u = u + rot(r) * v - slope
                state[0, r] = u
                state[1, r] = v - rot(r) * u - rise
            else:
                state[0, r] = u + coef(r) * slope
                state[1, r] = v + rot(r) * u + coef(r) * rise

        prepare(0)
        for r in range(-LEAD, count + LEAD):
            if 0 <= r + LEAD < count:
                open_a(r + LEAD)
            if 0 <= r < count:
                close_a(r)
            if 0 <= r - LEAD < count:
                close_b(r - LEAD)
        return carry

    lax.fori_loop(0, STEPS, one, 0)


def over(count, body, block=8):
    trips = count // block

    def step(n, carry):
        body(n * block)
        return carry

    lax.fori_loop(0, trips, step, 0, unroll=2 if trips % 2 == 0 else 1)


def run(copies):
    for c in copies:
        c.start()
    for c in copies:
        c.wait()


def unfold(src, dst, row, sems, slot):
    columns, rows = dst.shape[-2], src.shape[-2]
    lead = (slice(None),) * (len(src.shape) - 2)
    return [
        pltpu.make_async_copy(
            src.at[lead + (slice(None), pl.ds(s * LANE, LANE))],
            dst.at[lead + (pl.ds(row, rows), s)],
            sems.at[slot + s],
        )
        for s in range(columns)
    ]


def pack_kernel(own, mid, far, southward, northward):
    for src, rows, at in ((own, NEAR, 0), (mid, FAR, NEAR), (far, NEAR, NEAR + FAR)):
        last = src.shape[1] - rows
        southward[:, pl.ds(at, rows)] = src[:, pl.ds(last, rows)]
        northward[:, pl.ds(at, rows)] = src[:, pl.ds(0, rows)]


def fixed_kernel(weight, depth, southward, northward, sems):
    parts, rows, _ = weight.shape
    copies = []
    for k, (dst, w, d) in enumerate(((southward, rows - EDGE_W, rows - FAR), (northward, 0, 0))):
        moves = [
            (weight.at[p, pl.ds(w, EDGE_W)], dst.at[pl.ds(p * EDGE_W, EDGE_W)])
            for p in range(parts)
        ]
        moves.append((depth.at[pl.ds(d, FAR)], dst.at[pl.ds(parts * EDGE_W, FAR)]))
        for n, (src, out) in enumerate(moves):
            copies.append(pltpu.make_async_copy(src, out, sems.at[k * (parts + 1) + n]))
    run(copies)


def round_kernel(
    finish,
    own_lo,
    flags,
    own_e,
    own_m,
    mid_e,
    mid_m,
    far_e,
    far_m,
    from_north,
    from_south,
    start,
    depth,
    rate,
    weight,
    fixed_n,
    fixed_s,
    obs_a,
    obs_b,
    *refs,
):
    outs, cost_out = refs[:finish], refs[finish]
    lo, mid, kept, hi, depth_v, rate_v, weight_v, a_v, b_v, cost_v, sems, wide_sems = refs[
        finish + 1 :
    ]
    rows = kept.shape[1]
    inner = rows - 2 * FAR
    columns = kept.shape[2]

    def assemble(dst, halo, e, m, at, slot):
        pieces = [
            (from_north.at[:, pl.ds(at, halo)], 0, halo),
            (e.at[:, pl.ds(0, FAR)], halo, FAR),
            (m, halo + FAR, inner),
            (e.at[:, pl.ds(FAR, FAR)], halo + FAR + inner, FAR),
            (from_south.at[:, pl.ds(at, halo)], halo + rows, halo),
        ]
        return [
            pltpu.make_async_copy(src, dst.at[:, pl.ds(where, length)], sems.at[slot + n])
            for n, (src, where, length) in enumerate(pieces)
        ]

    own_at, mid_at, far_at = 0, NEAR, NEAR + FAR
    is_own_lo = own_lo[0] == 1
    c_rate = pltpu.make_async_copy(rate, rate_v, sems.at[0])
    c_mid = assemble(mid, FAR, mid_e, mid_m, mid_at, 2)
    lo_own = assemble(lo, NEAR, own_e, own_m, own_at, 7)
    lo_far = assemble(lo, NEAR, far_e, far_m, far_at, 7)
    hi_own = assemble(hi, NEAR, own_e, own_m, own_at, 12)
    hi_far = assemble(hi, NEAR, far_e, far_m, far_at, 12)
    c_kept = [
        pltpu.make_async_copy(mid_e.at[:, pl.ds(0, FAR)], kept.at[:, pl.ds(0, FAR)], sems.at[17]),
        pltpu.make_async_copy(mid_m, kept.at[:, pl.ds(FAR, inner)], sems.at[18]),
        pltpu.make_async_copy(
            mid_e.at[:, pl.ds(FAR, FAR)], kept.at[:, pl.ds(FAR + inner, FAR)], sems.at[19]
        ),
    ]
    c_a = pltpu.make_async_copy(obs_a, a_v, sems.at[20])
    c_b = pltpu.make_async_copy(obs_b, b_v, sems.at[21])
    c_depth = unfold(depth, depth_v, FAR, wide_sems, 0)
    c_weight = unfold(weight, weight_v, EDGE_W, wide_sems, columns)
    for n, (fixed, top_d, top_w) in enumerate(
        ((fixed_n, 0, 0), (fixed_s, FAR + rows, EDGE_W + rows))
    ):
        slot = (2 + 4 * n) * columns
        for p in range(3):
            c_weight += unfold(
                fixed.at[pl.ds(p * EDGE_W, EDGE_W)],
                weight_v.at[p],
                top_w,
                wide_sems,
                slot + p * columns,
            )
        c_depth += unfold(
            fixed.at[pl.ds(3 * EDGE_W, FAR)], depth_v, top_d, wide_sems, slot + 3 * columns
        )
    for c in c_depth + [c_rate] + c_mid:
        c.start()

    @pl.when(is_own_lo)
    def _():
        for c in lo_own + hi_far:
            c.start()

    @pl.when(jnp.logical_not(is_own_lo))
    def _():
        for c in lo_far + hi_own:
            c.start()

    for c in c_weight + c_kept + [c_a, c_b]:
        c.start()

    def scale_third(ref, where, length, block):
        def body(n):
            at = pl.ds(where + n, block)
            ref[2, at] = ref[2, at] * HALF

        over(length, body, block)

    for c in c_depth + [c_rate]:
        c.wait()

    def scale_depth(n):
        depth_v[pl.ds(n, 8)] = depth_v[pl.ds(n, 8)] * (HALF * HALF)

    over(depth_v.shape[0], scale_depth)
    for c in c_mid:
        c.wait()

    scale_third(mid, 0, mid.shape[1], 8)
    sweep(mid, depth_v, rate_v, 0, FAR, flags, True)
    for c in lo_own:
        c.wait()

    scale_third(lo, 0, lo.shape[1], 8)
    sweep(lo, depth_v, rate_v, FAR - NEAR, NEAR, flags, True)
    for c in hi_own + c_weight:
        c.wait()

    shift = EDGE_W - NEAR
    for part in range(3):
        back_scale = 1.0 / HALF if part == 2 else 1.0

        def body(n):
            at = pl.ds(n, 8)
            end = mid[part, pl.ds(FAR - NEAR + n, 8)] * back_scale
            lam = weight_v[part, pl.ds(shift + n, 8)] * (hi[part, at] - end)
            hi[part, at] = lam * (flags[2] * back_scale)

        over(hi.shape[1], body)

    for c in c_kept + [c_a, c_b]:
        c.wait()

    @pl.when(flags[3] > 0.5)
    def _():
        run(unfold(start, lo, NEAR, wide_sems, 0))
        scale_third(lo, NEAR, rows, 8)

    cost_v[...] = jnp.zeros_like(cost_v)
    for part in range(3):
        back_scale = 1.0 / HALF if part == 2 else 1.0

        def body(n):
            at = pl.ds(n, 8)
            here = kept[part, at]
            gap = here - lo[part, pl.ds(NEAR + n, 8)] * back_scale
            lam = weight_v[part, pl.ds(EDGE_W + n, 8)] * gap
            pull = a_v[part, at] * here
            kept[part, at] = here - STEP_SIZE * (lam + (pull - b_v[part, at]))
            cost_v[...] += lam * gap + here * (pull - 2.0 * b_v[part, at])

        over(rows, body)

    total = cost_v[0]
    for n in range(1, cost_v.shape[0]):
        total = total + cost_v[n]
    cost_out[...] = total

    sweep(hi, depth_v, rate_v, FAR - NEAR, NEAR, flags, False)
    copies = []
    for part in range(3):
        scale = STEP_SIZE * (HALF if part == 2 else 1.0)

        def add(n):
            at = pl.ds(n, 8)
            kept[part, at] = kept[part, at] + scale * hi[part, pl.ds(NEAR + n, 8)]

        over(rows, add)
        if finish == 2:
            moves = [
                (kept.at[part, pl.ds(0, FAR)], outs[0].at[part, pl.ds(0, FAR)]),
                (kept.at[part, pl.ds(rows - FAR, FAR)], outs[0].at[part, pl.ds(FAR, FAR)]),
                (kept.at[part, pl.ds(FAR, inner)], outs[1].at[part]),
            ]
        else:
            moves = [
                (kept.at[part, :, s], outs[0].at[part, :, pl.ds(s * LANE, LANE)])
                for s in range(columns)
            ]
        for n, (src, dst) in enumerate(moves):
            copies.append(pltpu.make_async_copy(src, dst, wide_sems.at[part * columns + n]))
            copies[-1].start()
    for c in copies:
        c.wait()


def deposit_kernel(plane, place, entries, a_out, b_out, const_out, *refs):
    words_v, words, picked, sems = refs[:4]
    values_v, values = refs[4:6]
    acc = refs[6:]
    a_acc, b_acc = acc[:GROUPS], acc[GROUPS:]
    comps, rows, columns, _ = a_out.shape
    lon = columns * LANE
    shift = lon.bit_length() - 1
    count, lanes = entries.shape[1:]
    spare = comps * rows

    index = entries[0].astype(jnp.int32)
    part = jnp.zeros_like(index)
    for n in range(1, comps):
        part = part + (index >= n * plane).astype(jnp.int32)
    rest = index - part * plane
    local = (rest >> shift) - place[0]
    kept = (index >= 0) & (local >= 0) & (local < rows)
    kept_f = kept.astype(jnp.float32)
    load = entries[2] * kept_f
    pulled = load * entries[1]
    row = lax.broadcasted_iota(jnp.int32, (lanes, lanes), 0)
    col = lax.broadcasted_iota(jnp.int32, (lanes, lanes), 1)
    before = (row < col).astype(jnp.float32)
    row = lax.broadcasted_iota(jnp.int32, (count, count), 0)
    col = lax.broadcasted_iota(jnp.int32, (count, count), 1)
    above = (col < row).astype(jnp.float32)
    dot = functools.partial(jnp.dot, preferred_element_type=jnp.float32)
    found = dot(kept_f, before) + dot(dot(above, kept_f), jnp.ones((lanes, lanes), jnp.float32))
    words_v[0] = found.astype(jnp.int32)
    words_v[1] = jnp.where(kept, ((part * rows + local) << shift) + (rest & (lon - 1)), spare << shift)
    values_v[0] = load
    values_v[1] = pulled
    const_out[...] = jnp.sum(
        (pulled * entries[1]).reshape(count // SUB, SUB, lanes), axis=0
    )
    copies = [
        pltpu.make_async_copy(words_v, words, sems.at[0]),
        pltpu.make_async_copy(values_v, values, sems.at[1]),
    ]
    for c in copies:
        c.start()

    zero = jnp.zeros((8, columns, LANE), jnp.float32)

    def clear(n):
        for ref in acc:
            ref[pl.ds(n, 8)] = zero

    over(spare, clear)
    column = lax.broadcasted_iota(jnp.int32, (columns, LANE), 0) * LANE
    column = column + lax.broadcasted_iota(jnp.int32, (columns, LANE), 1)
    for c in copies:
        c.wait()

    def pick(n, carry):
        for k in range(lanes):
            picked[words[0, n, k]] = n * lanes + k
        return carry

    lax.fori_loop(0, count, pick, 0)
    live = words[0, count - 1, lanes - 1]
    live = live + (words[1, count - 1, lanes - 1] < (spare << shift)).astype(jnp.int32)
    step = GROUPS * DEALS

    def body(n, carry):
        for k in range(DEALS):
            for g in range(GROUPS):
                at = n * step + (k * GROUPS + g)
                i = jnp.where(at < live, picked[at], 0)
                r, c = i >> (lanes.bit_length() - 1), i & (lanes - 1)
                word = jnp.where(at < live, words[1, r, c], spare << shift)
                hit = column == (word & (lon - 1))
                to = word >> shift
                a_acc[g][to] = a_acc[g][to] + jnp.where(hit, values[0, r, c], 0.0)
                b_acc[g][to] = b_acc[g][to] + jnp.where(hit, values[1, r, c], 0.0)
        return carry

    lax.fori_loop(0, (live + step - 1) // step, body, 0)
    copies = []
    for n in range(comps):

        def total(r):
            at = pl.ds(n * rows + r, 8)
            for group in (a_acc, b_acc):
                group[0][at] = (group[0][at] + group[1][at]) + (group[2][at] + group[3][at])

        over(rows, total)
        for k, (out, group) in enumerate(((a_out, a_acc), (b_out, b_acc))):
            copies.append(
                pltpu.make_async_copy(
                    group[0].at[pl.ds(n * rows, rows)], out.at[n], sems.at[2 + 2 * n + k]
                )
            )
            copies[-1].start()
    for c in copies:
        c.wait()


def per_device(
    increments, start_state, depth, error_weight, obs_index, obs_count, obs_value, obs_weight
):
    _, comps, rows, lon = increments.shape
    bands = lax.axis_size("space")
    windows = lax.axis_size("tm")
    band = lax.axis_index("space")
    me = lax.axis_index("tm")
    even = me % 2 == 0
    total_rows = rows * bands
    first_row = band * rows
    columns = lon // LANE
    f32 = jnp.float32
    hbm = pl.BlockSpec(memory_space=pltpu.HBM)
    smem = pl.BlockSpec(memory_space=pltpu.SMEM)
    vmem = pl.BlockSpec(memory_space=pltpu.VMEM)

    swap = [(i, i ^ 1) for i in range(windows)]
    inward = [(i, i - 2) for i in range(2, windows) if i % 2 == 0] + [
        (i, i + 2) for i in range(windows - 2) if i % 2 == 1
    ]
    outward = [(b, a) for a, b in inward]
    southward = [(i, i + 1) for i in range(bands - 1)]
    northward = [(b, a) for a, b in southward]

    own = increments[0].reshape(comps, rows, columns, LANE)
    edge = jnp.concatenate([own[:, :FAR], own[:, rows - FAR :]], 1)
    inner = own[:, FAR : rows - FAR]

    number = obs_index.shape[1]
    index = jnp.where(jnp.arange(number) < obs_count[0], obs_index[0], -1).astype(f32)
    own_list = jnp.stack([index, obs_value[0], obs_weight[0]])
    own_list = own_list.reshape(3, number // LANE, LANE)
    other_list = lax.ppermute(own_list, "tm", swap)

    def kernel(body, in_specs, out_specs, outs, scratch, flops):
        return pl.pallas_call(
            body,
            in_specs=in_specs,
            out_specs=out_specs,
            out_shape=outs,
            scratch_shapes=scratch,
            cost_estimate=pl.CostEstimate(flops=flops, bytes_accessed=0, transcendentals=0),
        )

    def field(*shape):
        return jax.ShapeDtypeStruct(shape + (columns, LANE), f32)

    def held(*shape):
        return pltpu.VMEM(shape + (columns, LANE), f32)

    tile = jax.ShapeDtypeStruct((SUB, LANE), f32)
    list_shape = own_list.shape[1:]
    deposit = kernel(
        functools.partial(deposit_kernel, total_rows * lon),
        [smem, vmem],
        [hbm, hbm, vmem],
        [field(comps, rows), field(comps, rows), tile],
        [
            pltpu.VMEM((2,) + list_shape, jnp.int32),
            pltpu.SMEM((2,) + list_shape, jnp.int32),
            pltpu.SMEM((number + GROUPS * DEALS,), jnp.int32),
            pltpu.SemaphoreType.DMA((2 + 2 * comps,)),
            pltpu.VMEM((2,) + list_shape, f32),
            pltpu.SMEM((2,) + list_shape, f32),
        ]
        + [held(comps * rows + 1)] * (2 * GROUPS),
        20_000_000,
    )
    place = jnp.reshape(first_row, (1,)).astype(jnp.int32)

    latitude = (
        (first_row - FAR + jnp.arange(rows + 2 * FAR)).astype(f32) + 0.5
    ) / total_rows * math.pi - math.pi / 2
    rate_wide = jnp.broadcast_to(
        (CORIOLIS_MAX * jnp.sin(latitude))[:, None], (rows + 2 * FAR, LANE)
    )

    small = pltpu.CompilerParams(vmem_limit_bytes=12 << 20)
    pack = pl.pallas_call(
        pack_kernel,
        in_specs=[vmem] * 3,
        out_specs=[vmem] * 2,
        out_shape=[field(comps, 2 * NEAR + FAR)] * 2,
        compiler_params=small,
        name="pack",
    )
    fixed = pl.pallas_call(
        fixed_kernel,
        in_specs=[hbm] * 2,
        out_specs=[vmem] * 2,
        out_shape=[jax.ShapeDtypeStruct((comps * EDGE_W + FAR, lon), f32)] * 2,
        scratch_shapes=[pltpu.SemaphoreType.DMA((2 * (comps + 1),))],
        compiler_params=small,
        name="fixed",
    )
    to_south, to_north = fixed(error_weight, depth)
    fixed_n = lax.ppermute(to_south, "space", southward)
    fixed_s = lax.ppermute(to_north, "space", northward)

    def round_call(finish, outs):
        return kernel(
            functools.partial(round_kernel, finish),
            [smem, smem] + [hbm] * 16,
            [hbm] * finish + [vmem],
            outs + [tile],
            [
                held(comps, rows + 2 * NEAR),
                held(comps, rows + 2 * FAR),
                held(comps, rows),
                held(comps, rows + 2 * NEAR),
                held(rows + 2 * FAR),
                pltpu.VMEM((rows + 2 * FAR, LANE), f32),
                held(comps, rows + 2 * EDGE_W),
                held(comps, rows),
                held(comps, rows),
                held(8),
                pltpu.SemaphoreType.DMA((22,)),
                pltpu.SemaphoreType.DMA((10 * columns,)),
            ],
            45_000_000,
        )

    def ring_sum(x):
        total = x
        for turn in range(1, bands):
            ring = [(i, (i + turn) % bands) for i in range(bands)]
            total = total + lax.ppermute(x, "space", ring)
        return total

    for turn in range(ITERS):
        away = turn % 2 == 0
        target = (me ^ 1) if away else me
        shift = inward if away else outward
        mid_e = lax.ppermute(edge, "tm", swap)
        far_e = lax.ppermute(edge, "tm", shift)
        mid_m = lax.ppermute(inner, "tm", swap)
        far_m = lax.ppermute(inner, "tm", shift)
        if away:
            _, mid_e = lax.optimization_barrier((to_south, mid_e))
        to_south, to_north = pack(edge, mid_e, far_e)
        entries = other_list if away else own_list
        to_south, entries = lax.optimization_barrier((to_south, entries))
        obs_a, obs_b, const = deposit(place, entries)
        from_north = lax.ppermute(to_south, "space", southward)
        from_south = lax.ppermute(to_north, "space", northward)
        own_lo = (even if away else ~even).astype(jnp.int32).reshape(1)
        flags = jnp.stack(
            [band > 0, band < bands - 1, target < windows - 1, target == 0]
        ).astype(f32)
        if turn < ITERS - 1:
            outs = [field(comps, 2 * FAR), field(comps, rows - 2 * FAR)]
        else:
            outs = [jax.ShapeDtypeStruct((comps, rows, lon), f32)]
        *state, cost = round_call(len(outs), outs)(
            own_lo,
            flags,
            edge,
            inner,
            mid_e,
            mid_m,
            far_e,
            far_m,
            from_north,
            from_south,
            start_state,
            depth,
            rate_wide,
            error_weight,
            fixed_n,
            fixed_s,
            obs_a,
            obs_b,
        )
        if turn == 0:
            edge, inner = state
            early = lax.ppermute(cost + const, "tm", swap)
    early, cost = lax.optimization_barrier((early, cost))
    sums = ring_sum(jnp.stack([early, cost + const]))
    cells = comps * total_rows * lon
    return state[0][None], (0.5 / cells) * jnp.sum(sums, (1, 2))[:, None]


def solution(mesh):
    placed = (
        P("tm", None, "space", None),
        P(None, "space", None),
        P("space", None),
        P(None, "space", None),
        P("tm", None),
        P("tm"),
        P("tm", None),
        P("tm", None),
    )

    return jax.shard_map(
        per_device,
        mesh=mesh,
        in_specs=placed,
        out_specs=(P("tm", None, "space", None), P(None, "tm")),
        check_vma=False,
    )
```

```python
import functools
import math

import jax
import jax.numpy as jnp
from jax import lax
from jax.experimental import pallas as pl
from jax.experimental.pallas import tpu as pltpu
from jax.sharding import PartitionSpec as P


STEPS = 6
ITERS = 2
COURANT = 0.35
CORIOLIS_MAX = 0.2
STEP_SIZE = 0.2

SUB = 8
LANE = 128
NEAR = 2 * STEPS
FAR = 4 * STEPS
GROUPS = 4
DEALS = 4
HALF = 0.5 * COURANT
LEAD = 24

EDGE_W = 16


def turned(x):
    return pltpu.roll(x, LANE - 1, 1), pltpu.roll(x, 1, 1)


def raw_lon(pair, first, last):
    ahead, behind = pair
    size = ahead.shape[0]
    ahead = jnp.where(last, pltpu.roll(ahead, size - 1, 0), ahead)
    behind = jnp.where(first, pltpu.roll(behind, 1, 0), behind)
    return ahead - behind


def sweep(state, depth, rate, off, halo, edge_ref, forward):
    count = rate.shape[0] - 2 * off
    north, south = halo - 1, count - halo

    def one(_, carry):
        lane = lax.broadcasted_iota(jnp.int32, depth.shape[1:], 1)
        first, last = lane == 0, lane == LANE - 1
        flows, tops, pairs_a, pairs_b = {}, {}, {}, {}

        def coef(r):
            return depth[off + r]

        def rot(r):
            return rate[pl.ds(off + r, 1), :]

        def masked(r, x):
            if r == north:
                return x * edge_ref[0]
            if r == south:
                return x * edge_ref[1]
            return x

        def prepare(r):
            v = state[1, r]
            flows[r] = coef(r) * v if forward else v

        def lat(values, r):
            return values[min(r + 1, count - 1)] - values[max(r - 1, 0)]

        def open_a(r):
            if forward:
                pairs_a[r] = turned(coef(r) * state[0, r])
            else:
                mix = state[0, r] - rot(r) * state[1, r]
                state[0, r] = mix
                pairs_a[r] = turned(mix)

        def close_a(r):
            if r + 1 < count:
                prepare(r + 1)
            slope = raw_lon(pairs_a.pop(r), first, last) + lat(flows, r)
            old = state[2, r]
            tops[r] = masked(r, old - slope if forward else old + slope)
            state[2, r] = tops[r]
            pairs_b[r] = turned(tops[r])

        def close_b(r):
            u, v = state[0, r], state[1, r]
            slope = raw_lon(pairs_b.pop(r), first, last)
            if r + 1 < count:
                above = state[2, r + 1]
            else:
                above = tops[r]
            rise = above - state[2, max(r - 1, 0)]
            if forward:
                u = u + rot(r) * v - slope
                state[0, r] = u
                state[1, r] = v - rot(r) * u - rise
            else:
                state[0, r] = u + coef(r) * slope
                state[1, r] = v + rot(r) * u + coef(r) * rise

        prepare(0)
        for r in range(-LEAD, count + LEAD):
            if 0 <= r + LEAD < count:
                open_a(r + LEAD)
            if 0 <= r < count:
                close_a(r)
            if 0 <= r - LEAD < count:
                close_b(r - LEAD)
        return carry

    lax.fori_loop(0, STEPS, one, 0)


def over(count, body, block=8):
    trips = count // block

    def step(n, carry):
        body(n * block)
        return carry

    lax.fori_loop(0, trips, step, 0, unroll=2 if trips % 2 == 0 else 1)


def run(copies):
    for c in copies:
        c.start()
    for c in copies:
        c.wait()


def unfold(src, dst, row, sems, slot):
    columns, rows = dst.shape[-2], src.shape[-2]
    lead = (slice(None),) * (len(src.shape) - 2)
    return [
        pltpu.make_async_copy(
            src.at[lead + (slice(None), pl.ds(s * LANE, LANE))],
            dst.at[lead + (pl.ds(row, rows), s)],
            sems.at[slot + s],
        )
        for s in range(columns)
    ]


def pack_kernel(own, mid, far, southward, northward):
    for src, rows, at in ((own, NEAR, 0), (mid, FAR, NEAR), (far, NEAR, NEAR + FAR)):
        last = src.shape[1] - rows
        southward[:, pl.ds(at, rows)] = src[:, pl.ds(last, rows)]
        northward[:, pl.ds(at, rows)] = src[:, pl.ds(0, rows)]


def fixed_kernel(weight, depth, southward, northward, sems):
    parts, rows, _ = weight.shape
    copies = []
    for k, (dst, w, d) in enumerate(((southward, rows - EDGE_W, rows - FAR), (northward, 0, 0))):
        moves = [
            (weight.at[p, pl.ds(w, EDGE_W)], dst.at[pl.ds(p * EDGE_W, EDGE_W)])
            for p in range(parts)
        ]
        moves.append((depth.at[pl.ds(d, FAR)], dst.at[pl.ds(parts * EDGE_W, FAR)]))
        for n, (src, out) in enumerate(moves):
            copies.append(pltpu.make_async_copy(src, out, sems.at[k * (parts + 1) + n]))
    run(copies)


def round_kernel(
    finish,
    own_lo,
    flags,
    own_e,
    own_m,
    mid_e,
    mid_m,
    far_e,
    far_m,
    from_north,
    from_south,
    start,
    depth,
    rate,
    weight,
    fixed_n,
    fixed_s,
    obs_a,
    obs_b,
    *refs,
):
    outs, cost_out = refs[:finish], refs[finish]
    lo, mid, kept, hi, depth_v, rate_v, weight_v, a_v, b_v, cost_v, sems, wide_sems = refs[
        finish + 1 :
    ]
    rows = kept.shape[1]
    inner = rows - 2 * FAR
    columns = kept.shape[2]

    def assemble(dst, halo, e, m, at, slot):
        pieces = [
            (from_north.at[:, pl.ds(at, halo)], 0, halo),
            (e.at[:, pl.ds(0, FAR)], halo, FAR),
            (m, halo + FAR, inner),
            (e.at[:, pl.ds(FAR, FAR)], halo + FAR + inner, FAR),
            (from_south.at[:, pl.ds(at, halo)], halo + rows, halo),
        ]
        return [
            pltpu.make_async_copy(src, dst.at[:, pl.ds(where, length)], sems.at[slot + n])
            for n, (src, where, length) in enumerate(pieces)
        ]

    own_at, mid_at, far_at = 0, NEAR, NEAR + FAR
    is_own_lo = own_lo[0] == 1
    c_rate = pltpu.make_async_copy(rate, rate_v, sems.at[0])
    c_mid = assemble(mid, FAR, mid_e, mid_m, mid_at, 2)
    lo_own = assemble(lo, NEAR, own_e, own_m, own_at, 7)
    lo_far = assemble(lo, NEAR, far_e, far_m, far_at, 7)
    hi_own = assemble(hi, NEAR, own_e, own_m, own_at, 12)
    hi_far = assemble(hi, NEAR, far_e, far_m, far_at, 12)
    c_kept = [
        pltpu.make_async_copy(mid_e.at[:, pl.ds(0, FAR)], kept.at[:, pl.ds(0, FAR)], sems.at[17]),
        pltpu.make_async_copy(mid_m, kept.at[:, pl.ds(FAR, inner)], sems.at[18]),
        pltpu.make_async_copy(
            mid_e.at[:, pl.ds(FAR, FAR)], kept.at[:, pl.ds(FAR + inner, FAR)], sems.at[19]
        ),
    ]
    c_a = pltpu.make_async_copy(obs_a, a_v, sems.at[20])
    c_b = pltpu.make_async_copy(obs_b, b_v, sems.at[21])
    c_depth = unfold(depth, depth_v, FAR, wide_sems, 0)
    c_weight = unfold(weight, weight_v, EDGE_W, wide_sems, columns)
    for n, (fixed, top_d, top_w) in enumerate(
        ((fixed_n, 0, 0), (fixed_s, FAR + rows, EDGE_W + rows))
    ):
        slot = (2 + 4 * n) * columns
        for p in range(3):
            c_weight += unfold(
                fixed.at[pl.ds(p * EDGE_W, EDGE_W)],
                weight_v.at[p],
                top_w,
                wide_sems,
                slot + p * columns,
            )
        c_depth += unfold(
            fixed.at[pl.ds(3 * EDGE_W, FAR)], depth_v, top_d, wide_sems, slot + 3 * columns
        )
    for c in c_depth + [c_rate] + c_mid:
        c.start()

    @pl.when(is_own_lo)
    def _():
        for c in lo_own + hi_far:
            c.start()

    @pl.when(jnp.logical_not(is_own_lo))
    def _():
        for c in lo_far + hi_own:
            c.start()

    for c in c_weight + c_kept + [c_a, c_b]:
        c.start()

    def scale_third(ref, where, length, block):
        def body(n):
            at = pl.ds(where + n, block)
            ref[2, at] = ref[2, at] * HALF

        over(length, body, block)

    for c in c_depth + [c_rate]:
        c.wait()

    def scale_depth(n):
        depth_v[pl.ds(n, 8)] = depth_v[pl.ds(n, 8)] * (HALF * HALF)

    over(depth_v.shape[0], scale_depth)
    for c in c_mid:
        c.wait()

    scale_third(mid, 0, mid.shape[1], 8)
    sweep(mid, depth_v, rate_v, 0, FAR, flags, True)
    for c in lo_own:
        c.wait()

    scale_third(lo, 0, lo.shape[1], 8)
    sweep(lo, depth_v, rate_v, FAR - NEAR, NEAR, flags, True)
    for c in hi_own + c_weight:
        c.wait()

    shift = EDGE_W - NEAR
    for part in range(3):
        back_scale = 1.0 / HALF if part == 2 else 1.0

        def body(n):
            at = pl.ds(n, 8)
            end = mid[part, pl.ds(FAR - NEAR + n, 8)] * back_scale
            lam = weight_v[part, pl.ds(shift + n, 8)] * (hi[part, at] - end)
            hi[part, at] = lam * (flags[2] * back_scale)

        over(hi.shape[1], body)

    for c in c_kept + [c_a, c_b]:
        c.wait()

    @pl.when(flags[3] > 0.5)
    def _():
        run(unfold(start, lo, NEAR, wide_sems, 0))
        scale_third(lo, NEAR, rows, 8)

    cost_v[...] = jnp.zeros_like(cost_v)
    for part in range(3):
        back_scale = 1.0 / HALF if part == 2 else 1.0

        def body(n):
            at = pl.ds(n, 8)
            here = kept[part, at]
            gap = here - lo[part, pl.ds(NEAR + n, 8)] * back_scale
            lam = weight_v[part, pl.ds(EDGE_W + n, 8)] * gap
            pull = a_v[part, at] * here
            kept[part, at] = here - STEP_SIZE * (lam + (pull - b_v[part, at]))
            cost_v[...] += lam * gap + here * (pull - 2.0 * b_v[part, at])

        over(rows, body)

    total = cost_v[0]
    for n in range(1, cost_v.shape[0]):
        total = total + cost_v[n]
    cost_out[...] = total

    sweep(hi, depth_v, rate_v, FAR - NEAR, NEAR, flags, False)
    copies = []
    for part in range(3):
        scale = STEP_SIZE * (HALF if part == 2 else 1.0)

        def add(n):
            at = pl.ds(n, 8)
            kept[part, at] = kept[part, at] + scale * hi[part, pl.ds(NEAR + n, 8)]

        over(rows, add)
        if finish == 2:
            moves = [
                (kept.at[part, pl.ds(0, FAR)], outs[0].at[part, pl.ds(0, FAR)]),
                (kept.at[part, pl.ds(rows - FAR, FAR)], outs[0].at[part, pl.ds(FAR, FAR)]),
                (kept.at[part, pl.ds(FAR, inner)], outs[1].at[part]),
            ]
        else:
            moves = [
                (kept.at[part, :, s], outs[0].at[part, :, pl.ds(s * LANE, LANE)])
                for s in range(columns)
            ]
        for n, (src, dst) in enumerate(moves):
            copies.append(pltpu.make_async_copy(src, dst, wide_sems.at[part * columns + n]))
            copies[-1].start()
    for c in copies:
        c.wait()


def deposit_kernel(plane, place, entries, a_out, b_out, const_out, *refs):
    words_v, words, picked, sems = refs[:4]
    values_v, values = refs[4:6]
    acc = refs[6:]
    a_acc, b_acc = acc[:GROUPS], acc[GROUPS:]
    comps, rows, columns, _ = a_out.shape
    lon = columns * LANE
    shift = lon.bit_length() - 1
    count, lanes = entries.shape[1:]
    spare = comps * rows

    index = entries[0].astype(jnp.int32)
    part = jnp.zeros_like(index)
    for n in range(1, comps):
        part = part + (index >= n * plane).astype(jnp.int32)
    rest = index - part * plane
    local = (rest >> shift) - place[0]
    kept = (index >= 0) & (local >= 0) & (local < rows)
    kept_f = kept.astype(jnp.float32)
    load = entries[2] * kept_f
    pulled = load * entries[1]
    row = lax.broadcasted_iota(jnp.int32, (lanes, lanes), 0)
    col = lax.broadcasted_iota(jnp.int32, (lanes, lanes), 1)
    before = (row < col).astype(jnp.float32)
    row = lax.broadcasted_iota(jnp.int32, (count, count), 0)
    col = lax.broadcasted_iota(jnp.int32, (count, count), 1)
    above = (col < row).astype(jnp.float32)
    dot = functools.partial(jnp.dot, preferred_element_type=jnp.float32)
    found = dot(kept_f, before) + dot(dot(above, kept_f), jnp.ones((lanes, lanes), jnp.float32))
    words_v[0] = found.astype(jnp.int32)
    words_v[1] = jnp.where(kept, ((part * rows + local) << shift) + (rest & (lon - 1)), spare << shift)
    values_v[0] = load
    values_v[1] = pulled
    const_out[...] = jnp.sum(
        (pulled * entries[1]).reshape(count // SUB, SUB, lanes), axis=0
    )
    copies = [
        pltpu.make_async_copy(words_v, words.at[:, pl.ds(0, count)], sems.at[0]),
        pltpu.make_async_copy(values_v, values.at[:, pl.ds(0, count)], sems.at[1]),
    ]
    for c in copies:
        c.start()

    zero = jnp.zeros((8, columns, LANE), jnp.float32)

    def clear(n):
        for ref in acc:
            ref[pl.ds(n, 8)] = zero

    over(spare, clear)
    column = lax.broadcasted_iota(jnp.int32, (columns, LANE), 0) * LANE
    column = column + lax.broadcasted_iota(jnp.int32, (columns, LANE), 1)
    for c in copies:
        c.wait()

    def pick(n, carry):
        for k in range(lanes):
            picked[words[0, n, k]] = n * lanes + k
        return carry

    lax.fori_loop(0, count, pick, 0)
    live = words[0, count - 1, lanes - 1]
    live = live + (words[1, count - 1, lanes - 1] < (spare << shift)).astype(jnp.int32)
    step = GROUPS * DEALS
    words[1, count, 0] = spare << shift
    values[0, count, 0] = 0.0
    values[1, count, 0] = 0.0
    for k in range(step):
        picked[live + k] = count * lanes

    def body(n, carry):
        for k in range(DEALS):
            for g in range(GROUPS):
                i = picked[n * step + (k * GROUPS + g)]
                r, c = i >> (lanes.bit_length() - 1), i & (lanes - 1)
                word = words[1, r, c]
                hit = column == (word & (lon - 1))
                to = word >> shift
                a_acc[g][to] = a_acc[g][to] + jnp.where(hit, values[0, r, c], 0.0)
                b_acc[g][to] = b_acc[g][to] + jnp.where(hit, values[1, r, c], 0.0)
        return carry

    lax.fori_loop(0, (live + step - 1) // step, body, 0)
    copies = []
    for n in range(comps):

        def total(r):
            at = pl.ds(n * rows + r, 8)
            for group in (a_acc, b_acc):
                group[0][at] = (group[0][at] + group[1][at]) + (group[2][at] + group[3][at])

        over(rows, total)
        for k, (out, group) in enumerate(((a_out, a_acc), (b_out, b_acc))):
            copies.append(
                pltpu.make_async_copy(
                    group[0].at[pl.ds(n * rows, rows)], out.at[n], sems.at[2 + 2 * n + k]
                )
            )
            copies[-1].start()
    for c in copies:
        c.wait()


def per_device(
    increments, start_state, depth, error_weight, obs_index, obs_count, obs_value, obs_weight
):
    _, comps, rows, lon = increments.shape
    bands = lax.axis_size("space")
    windows = lax.axis_size("tm")
    band = lax.axis_index("space")
    me = lax.axis_index("tm")
    even = me % 2 == 0
    total_rows = rows * bands
    first_row = band * rows
    columns = lon // LANE
    f32 = jnp.float32
    hbm = pl.BlockSpec(memory_space=pltpu.HBM)
    smem = pl.BlockSpec(memory_space=pltpu.SMEM)
    vmem = pl.BlockSpec(memory_space=pltpu.VMEM)

    swap = [(i, i ^ 1) for i in range(windows)]
    inward = [(i, i - 2) for i in range(2, windows) if i % 2 == 0] + [
        (i, i + 2) for i in range(windows - 2) if i % 2 == 1
    ]
    outward = [(b, a) for a, b in inward]
    southward = [(i, i + 1) for i in range(bands - 1)]
    northward = [(b, a) for a, b in southward]

    own = increments[0].reshape(comps, rows, columns, LANE)
    edge = jnp.concatenate([own[:, :FAR], own[:, rows - FAR :]], 1)
    inner = own[:, FAR : rows - FAR]

    number = obs_index.shape[1]
    index = jnp.where(jnp.arange(number) < obs_count[0], obs_index[0], -1).astype(f32)
    own_list = jnp.stack([index, obs_value[0], obs_weight[0]])
    own_list = own_list.reshape(3, number // LANE, LANE)
    other_list = lax.ppermute(own_list, "tm", swap)

    def kernel(body, in_specs, out_specs, outs, scratch, flops):
        return pl.pallas_call(
            body,
            in_specs=in_specs,
            out_specs=out_specs,
            out_shape=outs,
            scratch_shapes=scratch,
            cost_estimate=pl.CostEstimate(flops=flops, bytes_accessed=0, transcendentals=0),
        )

    def field(*shape):
        return jax.ShapeDtypeStruct(shape + (columns, LANE), f32)

    def held(*shape):
        return pltpu.VMEM(shape + (columns, LANE), f32)

    tile = jax.ShapeDtypeStruct((SUB, LANE), f32)
    list_shape = own_list.shape[1:]
    deposit = kernel(
        functools.partial(deposit_kernel, total_rows * lon),
        [smem, vmem],
        [hbm, hbm, vmem],
        [field(comps, rows), field(comps, rows), tile],
        [
            pltpu.VMEM((2,) + list_shape, jnp.int32),
            pltpu.SMEM((2, list_shape[0] + SUB, LANE), jnp.int32),
            pltpu.SMEM((number + GROUPS * DEALS,), jnp.int32),
            pltpu.SemaphoreType.DMA((2 + 2 * comps,)),
            pltpu.VMEM((2,) + list_shape, f32),
            pltpu.SMEM((2, list_shape[0] + SUB, LANE), f32),
        ]
        + [held(comps * rows + 1)] * (2 * GROUPS),
        20_000_000,
    )
    place = jnp.reshape(first_row, (1,)).astype(jnp.int32)

    latitude = (
        (first_row - FAR + jnp.arange(rows + 2 * FAR)).astype(f32) + 0.5
    ) / total_rows * math.pi - math.pi / 2
    rate_wide = jnp.broadcast_to(
        (CORIOLIS_MAX * jnp.sin(latitude))[:, None], (rows + 2 * FAR, LANE)
    )

    small = pltpu.CompilerParams(vmem_limit_bytes=12 << 20)
    pack = pl.pallas_call(
        pack_kernel,
        in_specs=[vmem] * 3,
        out_specs=[vmem] * 2,
        out_shape=[field(comps, 2 * NEAR + FAR)] * 2,
        compiler_params=small,
        name="pack",
    )
    fixed = pl.pallas_call(
        fixed_kernel,
        in_specs=[hbm] * 2,
        out_specs=[vmem] * 2,
        out_shape=[jax.ShapeDtypeStruct((comps * EDGE_W + FAR, lon), f32)] * 2,
        scratch_shapes=[pltpu.SemaphoreType.DMA((2 * (comps + 1),))],
        compiler_params=small,
        name="fixed",
    )
    to_south, to_north = fixed(error_weight, depth)
    fixed_n = lax.ppermute(to_south, "space", southward)
    fixed_s = lax.ppermute(to_north, "space", northward)

    def round_call(finish, outs):
        return kernel(
            functools.partial(round_kernel, finish),
            [smem, smem] + [hbm] * 16,
            [hbm] * finish + [vmem],
            outs + [tile],
            [
                held(comps, rows + 2 * NEAR),
                held(comps, rows + 2 * FAR),
                held(comps, rows),
                held(comps, rows + 2 * NEAR),
                held(rows + 2 * FAR),
                pltpu.VMEM((rows + 2 * FAR, LANE), f32),
                held(comps, rows + 2 * EDGE_W),
                held(comps, rows),
                held(comps, rows),
                held(8),
                pltpu.SemaphoreType.DMA((22,)),
                pltpu.SemaphoreType.DMA((10 * columns,)),
            ],
            45_000_000,
        )

    def ring_sum(x):
        total = x
        for turn in range(1, bands):
            ring = [(i, (i + turn) % bands) for i in range(bands)]
            total = total + lax.ppermute(x, "space", ring)
        return total

    for turn in range(ITERS):
        away = turn % 2 == 0
        target = (me ^ 1) if away else me
        shift = inward if away else outward
        mid_e = lax.ppermute(edge, "tm", swap)
        far_e = lax.ppermute(edge, "tm", shift)
        mid_m = lax.ppermute(inner, "tm", swap)
        far_m = lax.ppermute(inner, "tm", shift)
        if away:
            _, mid_e = lax.optimization_barrier((to_south, mid_e))
            to_south, to_north = pack(edge, mid_e, far_e)
            to_south, other_list = lax.optimization_barrier((to_south, other_list))
            obs_a, obs_b, const = deposit(place, other_list)
        else:
            _, own_list = lax.optimization_barrier((edge, own_list))
            obs_a, obs_b, const = deposit(place, own_list)
            const, mid_e = lax.optimization_barrier((const, mid_e))
            to_south, to_north = pack(edge, mid_e, far_e)
        from_north = lax.ppermute(to_south, "space", southward)
        from_south = lax.ppermute(to_north, "space", northward)
        own_lo = (even if away else ~even).astype(jnp.int32).reshape(1)
        flags = jnp.stack(
            [band > 0, band < bands - 1, target < windows - 1, target == 0]
        ).astype(f32)
        if turn < ITERS - 1:
            outs = [field(comps, 2 * FAR), field(comps, rows - 2 * FAR)]
        else:
            outs = [jax.ShapeDtypeStruct((comps, rows, lon), f32)]
        *state, cost = round_call(len(outs), outs)(
            own_lo,
            flags,
            edge,
            inner,
            mid_e,
            mid_m,
            far_e,
            far_m,
            from_north,
            from_south,
            start_state,
            depth,
            rate_wide,
            error_weight,
            fixed_n,
            fixed_s,
            obs_a,
            obs_b,
        )
        if turn == 0:
            edge, inner = state
            early = lax.ppermute(cost + const, "tm", swap)
    early, cost = lax.optimization_barrier((early, cost))
    sums = ring_sum(jnp.stack([early, cost + const]))
    cells = comps * total_rows * lon
    return state[0][None], (0.5 / cells) * jnp.sum(sums, (1, 2))[:, None]


def solution(mesh):
    placed = (
        P("tm", None, "space", None),
        P(None, "space", None),
        P("space", None),
        P(None, "space", None),
        P("tm", None),
        P("tm"),
        P("tm", None),
        P("tm", None),
    )

    return jax.shard_map(
        per_device,
        mesh=mesh,
        in_specs=placed,
        out_specs=(P("tm", None, "space", None), P(None, "tm")),
        check_vma=False,
    )
```

```python
import functools
import math

import jax
import jax.numpy as jnp
from jax import lax
from jax.experimental import pallas as pl
from jax.experimental.pallas import tpu as pltpu
from jax.sharding import PartitionSpec as P


STEPS = 6
ITERS = 2
COURANT = 0.35
CORIOLIS_MAX = 0.2
STEP_SIZE = 0.2

SUB = 8
LANE = 128
NEAR = 2 * STEPS
FAR = 4 * STEPS
GROUPS = 2
DEALS = 8
HALF = 0.5 * COURANT
LEAD = 32
AT_ONCE = 2

EDGE_W = 16


def turned(x):
    return pltpu.roll(x, LANE - 1, 1), pltpu.roll(x, 1, 1)


def raw_lon(pair, first, last):
    ahead, behind = pair
    size = ahead.shape[0]
    ahead = jnp.where(last, pltpu.roll(ahead, size - 1, 0), ahead)
    behind = jnp.where(first, pltpu.roll(behind, 1, 0), behind)
    return ahead - behind


def sweep(state, depth, rate, off, halo, edge_ref, forward):
    count = rate.shape[0] - 2 * off
    north, south = halo - 1, count - halo

    def one(begin, end, _, carry):
        lane = lax.broadcasted_iota(jnp.int32, depth.shape[1:], 1)
        first, last = lane == 0, lane == LANE - 1
        flows, tops, pairs_a, pairs_b = {}, {}, {}, {}

        def coef(r):
            return depth[off + r]

        def rot(r):
            return rate[pl.ds(off + r, 1), :]

        def masked(r, x):
            if r == north:
                return x * edge_ref[0]
            if r == south:
                return x * edge_ref[1]
            return x

        def prepare(r):
            v = state[1, r]
            flows[r] = coef(r) * v if forward else v

        def lat(values, r):
            return values[min(r + 1, end - 1)] - values[max(r - 1, begin)]

        def open_a(r):
            if forward:
                pairs_a[r] = turned(coef(r) * state[0, r])
            else:
                pairs_a[r] = turned(state[0, r] - rot(r) * state[1, r])

        def close_a(r):
            if r + 1 < end:
                prepare(r + 1)
            slope = raw_lon(pairs_a.pop(r), first, last) + lat(flows, r)
            old = state[2, r]
            tops[r] = masked(r, old - slope if forward else old + slope)
            state[2, r] = tops[r]
            pairs_b[r] = turned(tops[r])

        def close_b(r):
            u, v = state[0, r], state[1, r]
            slope = raw_lon(pairs_b.pop(r), first, last)
            if r + 1 < end:
                above = state[2, r + 1]
            else:
                above = tops[r]
            rise = above - state[2, max(r - 1, begin)]
            if forward:
                u = u + rot(r) * v - slope
                state[0, r] = u
                state[1, r] = v - rot(r) * u - rise
            else:
                u = u - rot(r) * v
                state[0, r] = u + coef(r) * slope
                state[1, r] = v + rot(r) * u + coef(r) * rise

        prepare(begin)
        for r in range(begin - LEAD, end + LEAD):
            if begin <= r + LEAD < end:
                open_a(r + LEAD)
            if begin <= r < end:
                close_a(r)
            if begin <= r - LEAD < end:
                close_b(r - LEAD)
        return carry

    for n in range(0, STEPS, AT_ONCE):
        trips = min(AT_ONCE, STEPS - n)
        lax.fori_loop(0, trips, functools.partial(one, 2 * n, count - 2 * n), 0)


def over(count, body, block=8):
    trips = count // block

    def step(n, carry):
        body(n * block)
        return carry

    lax.fori_loop(0, trips, step, 0, unroll=2 if trips % 2 == 0 else 1)


def run(copies):
    for c in copies:
        c.start()
    for c in copies:
        c.wait()


def unfold(src, dst, row, sems, slot):
    columns, rows = dst.shape[-2], src.shape[-2]
    lead = (slice(None),) * (len(src.shape) - 2)
    return [
        pltpu.make_async_copy(
            src.at[lead + (slice(None), pl.ds(s * LANE, LANE))],
            dst.at[lead + (pl.ds(row, rows), s)],
            sems.at[slot + s],
        )
        for s in range(columns)
    ]


def pack_kernel(own, mid, far, southward, northward):
    for src, rows, at in ((own, NEAR, 0), (mid, FAR, NEAR), (far, NEAR, NEAR + FAR)):
        last = src.shape[1] - rows
        southward[:, pl.ds(at, rows)] = src[:, pl.ds(last, rows)]
        northward[:, pl.ds(at, rows)] = src[:, pl.ds(0, rows)]


def fixed_kernel(weight, depth, southward, northward, sems):
    parts, rows, _ = weight.shape
    copies = []
    for k, (dst, w, d) in enumerate(((southward, rows - EDGE_W, rows - FAR), (northward, 0, 0))):
        moves = [
            (weight.at[p, pl.ds(w, EDGE_W)], dst.at[pl.ds(p * EDGE_W, EDGE_W)])
            for p in range(parts)
        ]
        moves.append((depth.at[pl.ds(d, FAR)], dst.at[pl.ds(parts * EDGE_W, FAR)]))
        for n, (src, out) in enumerate(moves):
            copies.append(pltpu.make_async_copy(src, out, sems.at[k * (parts + 1) + n]))
    run(copies)


def round_kernel(
    finish,
    own_lo,
    flags,
    own_e,
    own_m,
    mid_e,
    mid_m,
    far_e,
    far_m,
    from_north,
    from_south,
    start,
    depth,
    rate,
    weight,
    fixed_n,
    fixed_s,
    obs_a,
    obs_b,
    *refs,
):
    outs, cost_out = refs[:finish], refs[finish]
    lo, mid, kept, hi, depth_v, rate_v, weight_v, a_v, b_v, cost_v, sems, wide_sems = refs[
        finish + 1 :
    ]
    rows = kept.shape[1]
    inner = rows - 2 * FAR
    columns = kept.shape[2]

    def assemble(dst, halo, e, m, at, slot):
        pieces = [
            (from_north.at[:, pl.ds(at, halo)], 0, halo),
            (e.at[:, pl.ds(0, FAR)], halo, FAR),
            (m, halo + FAR, inner),
            (e.at[:, pl.ds(FAR, FAR)], halo + FAR + inner, FAR),
            (from_south.at[:, pl.ds(at, halo)], halo + rows, halo),
        ]
        return [
            pltpu.make_async_copy(src, dst.at[:, pl.ds(where, length)], sems.at[slot + n])
            for n, (src, where, length) in enumerate(pieces)
        ]

    own_at, mid_at, far_at = 0, NEAR, NEAR + FAR
    is_own_lo = own_lo[0] == 1
    c_rate = pltpu.make_async_copy(rate, rate_v, sems.at[0])
    c_mid = assemble(mid, FAR, mid_e, mid_m, mid_at, 2)
    lo_own = assemble(lo, NEAR, own_e, own_m, own_at, 7)
    lo_far = assemble(lo, NEAR, far_e, far_m, far_at, 7)
    hi_own = assemble(hi, NEAR, own_e, own_m, own_at, 12)
    hi_far = assemble(hi, NEAR, far_e, far_m, far_at, 12)
    c_kept = [
        pltpu.make_async_copy(mid_e.at[:, pl.ds(0, FAR)], kept.at[:, pl.ds(0, FAR)], sems.at[17]),
        pltpu.make_async_copy(mid_m, kept.at[:, pl.ds(FAR, inner)], sems.at[18]),
        pltpu.make_async_copy(
            mid_e.at[:, pl.ds(FAR, FAR)], kept.at[:, pl.ds(FAR + inner, FAR)], sems.at[19]
        ),
    ]
    c_a = pltpu.make_async_copy(obs_a, a_v, sems.at[20])
    c_b = pltpu.make_async_copy(obs_b, b_v, sems.at[21])
    c_depth = unfold(depth, depth_v, FAR, wide_sems, 0)
    c_weight = unfold(weight, weight_v, EDGE_W, wide_sems, columns)
    for n, (fixed, top_d, top_w) in enumerate(
        ((fixed_n, 0, 0), (fixed_s, FAR + rows, EDGE_W + rows))
    ):
        slot = (2 + 4 * n) * columns
        for p in range(3):
            c_weight += unfold(
                fixed.at[pl.ds(p * EDGE_W, EDGE_W)],
                weight_v.at[p],
                top_w,
                wide_sems,
                slot + p * columns,
            )
        c_depth += unfold(
            fixed.at[pl.ds(3 * EDGE_W, FAR)], depth_v, top_d, wide_sems, slot + 3 * columns
        )
    for c in c_depth + [c_rate] + c_mid:
        c.start()

    @pl.when(is_own_lo)
    def _():
        for c in lo_own + hi_far:
            c.start()

    @pl.when(jnp.logical_not(is_own_lo))
    def _():
        for c in lo_far + hi_own:
            c.start()

    for c in c_weight + c_kept + [c_a, c_b]:
        c.start()

    def scale_third(ref, where, length, block):
        def body(n):
            at = pl.ds(where + n, block)
            ref[2, at] = ref[2, at] * HALF

        over(length, body, block)

    for c in c_depth + [c_rate]:
        c.wait()

    def scale_depth(n):
        depth_v[pl.ds(n, 8)] = depth_v[pl.ds(n, 8)] * (HALF * HALF)

    over(depth_v.shape[0], scale_depth)
    for c in c_mid:
        c.wait()

    scale_third(mid, 0, mid.shape[1], 8)
    sweep(mid, depth_v, rate_v, 0, FAR, flags, True)
    for c in lo_own:
        c.wait()

    scale_third(lo, 0, lo.shape[1], 8)
    sweep(lo, depth_v, rate_v, FAR - NEAR, NEAR, flags, True)
    for c in hi_own + c_weight:
        c.wait()

    shift = EDGE_W - NEAR
    for part in range(3):
        back_scale = 1.0 / HALF if part == 2 else 1.0

        def body(n):
            at = pl.ds(n, 8)
            end = mid[part, pl.ds(FAR - NEAR + n, 8)] * back_scale
            lam = weight_v[part, pl.ds(shift + n, 8)] * (hi[part, at] - end)
            hi[part, at] = lam * (flags[2] * back_scale)

        over(hi.shape[1], body)

    for c in c_kept + [c_a, c_b]:
        c.wait()

    @pl.when(flags[3] > 0.5)
    def _():
        run(unfold(start, lo, NEAR, wide_sems, 0))
        scale_third(lo, NEAR, rows, 8)

    cost_v[...] = jnp.zeros_like(cost_v)
    for part in range(3):
        back_scale = 1.0 / HALF if part == 2 else 1.0

        def body(n):
            at = pl.ds(n, 8)
            here = kept[part, at]
            gap = here - lo[part, pl.ds(NEAR + n, 8)] * back_scale
            lam = weight_v[part, pl.ds(EDGE_W + n, 8)] * gap
            pull = a_v[part, at] * here
            kept[part, at] = here - STEP_SIZE * (lam + (pull - b_v[part, at]))
            cost_v[...] += lam * gap + here * (pull - 2.0 * b_v[part, at])

        over(rows, body)

    total = cost_v[0]
    for n in range(1, cost_v.shape[0]):
        total = total + cost_v[n]
    cost_out[...] = total

    sweep(hi, depth_v, rate_v, FAR - NEAR, NEAR, flags, False)
    copies = []
    for part in range(3):
        scale = STEP_SIZE * (HALF if part == 2 else 1.0)

        def add(n):
            at = pl.ds(n, 8)
            kept[part, at] = kept[part, at] + scale * hi[part, pl.ds(NEAR + n, 8)]

        over(rows, add)
        if finish == 2:
            moves = [
                (kept.at[part, pl.ds(0, FAR)], outs[0].at[part, pl.ds(0, FAR)]),
                (kept.at[part, pl.ds(rows - FAR, FAR)], outs[0].at[part, pl.ds(FAR, FAR)]),
                (kept.at[part, pl.ds(FAR, inner)], outs[1].at[part]),
            ]
        else:
            moves = [
                (kept.at[part, :, s], outs[0].at[part, :, pl.ds(s * LANE, LANE)])
                for s in range(columns)
            ]
        for n, (src, dst) in enumerate(moves):
            copies.append(pltpu.make_async_copy(src, dst, wide_sems.at[part * columns + n]))
            copies[-1].start()
    for c in copies:
        c.wait()


def deposit_kernel(plane, place, entries, a_out, b_out, const_out, *refs):
    words_v, words, picked, sems = refs[:4]
    values_v, values = refs[4:6]
    acc = refs[6:]
    a_acc, b_acc = acc[:GROUPS], acc[GROUPS:]
    comps, rows, columns, _ = a_out.shape
    lon = columns * LANE
    shift = lon.bit_length() - 1
    count, lanes = entries.shape[1:]
    spare = comps * rows

    index = entries[0].astype(jnp.int32)
    part = jnp.zeros_like(index)
    for n in range(1, comps):
        part = part + (index >= n * plane).astype(jnp.int32)
    rest = index - part * plane
    local = (rest >> shift) - place[0]
    kept = (index >= 0) & (local >= 0) & (local < rows)
    kept_f = kept.astype(jnp.float32)
    load = entries[2] * kept_f
    pulled = load * entries[1]
    row = lax.broadcasted_iota(jnp.int32, (lanes, lanes), 0)
    col = lax.broadcasted_iota(jnp.int32, (lanes, lanes), 1)
    before = (row < col).astype(jnp.float32)
    row = lax.broadcasted_iota(jnp.int32, (count, count), 0)
    col = lax.broadcasted_iota(jnp.int32, (count, count), 1)
    above = (col < row).astype(jnp.float32)
    dot = functools.partial(jnp.dot, preferred_element_type=jnp.float32)
    found = dot(kept_f, before) + dot(dot(above, kept_f), jnp.ones((lanes, lanes), jnp.float32))
    words_v[0] = found.astype(jnp.int32)
    words_v[1] = jnp.where(kept, ((part * rows + local) << shift) + (rest & (lon - 1)), spare << shift)
    values_v[0] = load
    values_v[1] = pulled
    const_out[...] = jnp.sum(
        (pulled * entries[1]).reshape(count // SUB, SUB, lanes), axis=0
    )
    copies = [
        pltpu.make_async_copy(words_v, words.at[:, pl.ds(0, count)], sems.at[0]),
        pltpu.make_async_copy(values_v, values.at[:, pl.ds(0, count)], sems.at[1]),
    ]
    for c in copies:
        c.start()

    zero = jnp.zeros((8, columns, LANE), jnp.float32)

    def clear(n):
        for ref in acc:
            ref[pl.ds(n, 8)] = zero

    over(spare, clear)
    column = lax.broadcasted_iota(jnp.int32, (columns, LANE), 0) * LANE
    column = column + lax.broadcasted_iota(jnp.int32, (columns, LANE), 1)
    for c in copies:
        c.wait()

    def pick(n, carry):
        for k in range(lanes):
            picked[words[0, n, k]] = n * lanes + k
        return carry

    lax.fori_loop(0, count, pick, 0)
    live = words[0, count - 1, lanes - 1]
    live = live + (words[1, count - 1, lanes - 1] < (spare << shift)).astype(jnp.int32)
    step = GROUPS * DEALS
    words[1, count, 0] = spare << shift
    values[0, count, 0] = 0.0
    values[1, count, 0] = 0.0
    for k in range(step):
        picked[live + k] = count * lanes

    def body(n, carry):
        for k in range(DEALS):
            for g in range(GROUPS):
                i = picked[n * step + (k * GROUPS + g)]
                r, c = i >> (lanes.bit_length() - 1), i & (lanes - 1)
                word = words[1, r, c]
                hit = column == (word & (lon - 1))
                to = word >> shift
                a_acc[g][to] = a_acc[g][to] + jnp.where(hit, values[0, r, c], 0.0)
                b_acc[g][to] = b_acc[g][to] + jnp.where(hit, values[1, r, c], 0.0)
        return carry

    lax.fori_loop(0, (live + step - 1) // step, body, 0)
    copies = []
    for n in range(comps):

        def total(r):
            at = pl.ds(n * rows + r, 8)
            for group in (a_acc, b_acc):
                group[0][at] = group[0][at] + group[1][at]

        over(rows, total)
        for k, (out, group) in enumerate(((a_out, a_acc), (b_out, b_acc))):
            copies.append(
                pltpu.make_async_copy(
                    group[0].at[pl.ds(n * rows, rows)], out.at[n], sems.at[2 + 2 * n + k]
                )
            )
            copies[-1].start()
    for c in copies:
        c.wait()


def per_device(
    increments, start_state, depth, error_weight, obs_index, obs_count, obs_value, obs_weight
):
    _, comps, rows, lon = increments.shape
    bands = lax.axis_size("space")
    windows = lax.axis_size("tm")
    band = lax.axis_index("space")
    me = lax.axis_index("tm")
    even = me % 2 == 0
    total_rows = rows * bands
    first_row = band * rows
    columns = lon // LANE
    f32 = jnp.float32
    hbm = pl.BlockSpec(memory_space=pltpu.HBM)
    smem = pl.BlockSpec(memory_space=pltpu.SMEM)
    vmem = pl.BlockSpec(memory_space=pltpu.VMEM)

    swap = [(i, i ^ 1) for i in range(windows)]
    inward = [(i, i - 2) for i in range(2, windows) if i % 2 == 0] + [
        (i, i + 2) for i in range(windows - 2) if i % 2 == 1
    ]
    outward = [(b, a) for a, b in inward]
    southward = [(i, i + 1) for i in range(bands - 1)]
    northward = [(b, a) for a, b in southward]

    own = increments[0].reshape(comps, rows, columns, LANE)
    edge = jnp.concatenate([own[:, :FAR], own[:, rows - FAR :]], 1)
    inner = own[:, FAR : rows - FAR]

    number = obs_index.shape[1]
    index = jnp.where(jnp.arange(number) < obs_count[0], obs_index[0], -1).astype(f32)
    own_list = jnp.stack([index, obs_value[0], obs_weight[0]])
    own_list = own_list.reshape(3, number // LANE, LANE)
    other_list = lax.ppermute(own_list, "tm", swap)

    def kernel(body, in_specs, out_specs, outs, scratch, flops):
        return pl.pallas_call(
            body,
            in_specs=in_specs,
            out_specs=out_specs,
            out_shape=outs,
            scratch_shapes=scratch,
            cost_estimate=pl.CostEstimate(flops=flops, bytes_accessed=0, transcendentals=0),
        )

    def field(*shape):
        return jax.ShapeDtypeStruct(shape + (columns, LANE), f32)

    def held(*shape):
        return pltpu.VMEM(shape + (columns, LANE), f32)

    tile = jax.ShapeDtypeStruct((SUB, LANE), f32)
    list_shape = own_list.shape[1:]
    deposit = kernel(
        functools.partial(deposit_kernel, total_rows * lon),
        [smem, vmem],
        [hbm, hbm, vmem],
        [field(comps, rows), field(comps, rows), tile],
        [
            pltpu.VMEM((2,) + list_shape, jnp.int32),
            pltpu.SMEM((2, list_shape[0] + SUB, LANE), jnp.int32),
            pltpu.SMEM((number + GROUPS * DEALS,), jnp.int32),
            pltpu.SemaphoreType.DMA((2 + 2 * comps,)),
            pltpu.VMEM((2,) + list_shape, f32),
            pltpu.SMEM((2, list_shape[0] + SUB, LANE), f32),
        ]
        + [held(comps * rows + 1)] * (2 * GROUPS),
        20_000_000,
    )
    place = jnp.reshape(first_row, (1,)).astype(jnp.int32)

    latitude = (
        (first_row - FAR + jnp.arange(rows + 2 * FAR)).astype(f32) + 0.5
    ) / total_rows * math.pi - math.pi / 2
    rate_wide = jnp.broadcast_to(
        (CORIOLIS_MAX * jnp.sin(latitude))[:, None], (rows + 2 * FAR, LANE)
    )

    small = pltpu.CompilerParams(vmem_limit_bytes=12 << 20)
    pack = pl.pallas_call(
        pack_kernel,
        in_specs=[vmem] * 3,
        out_specs=[vmem] * 2,
        out_shape=[field(comps, 2 * NEAR + FAR)] * 2,
        compiler_params=small,
        name="pack",
    )
    fixed = pl.pallas_call(
        fixed_kernel,
        in_specs=[hbm] * 2,
        out_specs=[vmem] * 2,
        out_shape=[jax.ShapeDtypeStruct((comps * EDGE_W + FAR, lon), f32)] * 2,
        scratch_shapes=[pltpu.SemaphoreType.DMA((2 * (comps + 1),))],
        compiler_params=small,
        name="fixed",
    )
    to_south, to_north = fixed(error_weight, depth)
    fixed_n = lax.ppermute(to_south, "space", southward)
    fixed_s = lax.ppermute(to_north, "space", northward)

    def round_call(finish, outs):
        return kernel(
            functools.partial(round_kernel, finish),
            [smem, smem] + [hbm] * 16,
            [hbm] * finish + [vmem],
            outs + [tile],
            [
                held(comps, rows + 2 * NEAR),
                held(comps, rows + 2 * FAR),
                held(comps, rows),
                held(comps, rows + 2 * NEAR),
                held(rows + 2 * FAR),
                pltpu.VMEM((rows + 2 * FAR, LANE), f32),
                held(comps, rows + 2 * EDGE_W),
                held(comps, rows),
                held(comps, rows),
                held(8),
                pltpu.SemaphoreType.DMA((22,)),
                pltpu.SemaphoreType.DMA((10 * columns,)),
            ],
            45_000_000,
        )

    def ring_sum(x):
        total = x
        for turn in range(1, bands):
            ring = [(i, (i + turn) % bands) for i in range(bands)]
            total = total + lax.ppermute(x, "space", ring)
        return total

    for turn in range(ITERS):
        away = turn % 2 == 0
        target = (me ^ 1) if away else me
        shift = inward if away else outward
        mid_e = lax.ppermute(edge, "tm", swap)
        far_e = lax.ppermute(edge, "tm", shift)
        mid_m = lax.ppermute(inner, "tm", swap)
        far_m = lax.ppermute(inner, "tm", shift)
        if away:
            fixed_n, fixed_s, mid_e = lax.optimization_barrier((fixed_n, fixed_s, mid_e))
            to_south, to_north = pack(edge, mid_e, far_e)
            to_south, other_list = lax.optimization_barrier((to_south, other_list))
            obs_a, obs_b, const = deposit(place, other_list)
        else:
            _, own_list = lax.optimization_barrier((edge, own_list))
            obs_a, obs_b, const = deposit(place, own_list)
            const, mid_e = lax.optimization_barrier((const, mid_e))
            to_south, to_north = pack(edge, mid_e, far_e)
        from_north = lax.ppermute(to_south, "space", southward)
        from_south = lax.ppermute(to_north, "space", northward)
        own_lo = (even if away else ~even).astype(jnp.int32).reshape(1)
        flags = jnp.stack(
            [band > 0, band < bands - 1, target < windows - 1, target == 0]
        ).astype(f32)
        if turn < ITERS - 1:
            outs = [field(comps, 2 * FAR), field(comps, rows - 2 * FAR)]
        else:
            outs = [jax.ShapeDtypeStruct((comps, rows, lon), f32)]
        *state, cost = round_call(len(outs), outs)(
            own_lo,
            flags,
            edge,
            inner,
            mid_e,
            mid_m,
            far_e,
            far_m,
            from_north,
            from_south,
            start_state,
            depth,
            rate_wide,
            error_weight,
            fixed_n,
            fixed_s,
            obs_a,
            obs_b,
        )
        if turn == 0:
            edge, inner = state
            early = lax.ppermute(cost + const, "tm", swap)
    early, cost = lax.optimization_barrier((early, cost))
    sums = ring_sum(jnp.stack([early, cost + const]))
    cells = comps * total_rows * lon
    return state[0][None], (0.5 / cells) * jnp.sum(sums, (1, 2))[:, None]


def solution(mesh):
    placed = (
        P("tm", None, "space", None),
        P(None, "space", None),
        P("space", None),
        P(None, "space", None),
        P("tm", None),
        P("tm"),
        P("tm", None),
        P("tm", None),
    )

    return jax.shard_map(
        per_device,
        mesh=mesh,
        in_specs=placed,
        out_specs=(P("tm", None, "space", None), P(None, "tm")),
        check_vma=False,
    )
```
